32 devices in a mesh: seq: 8 (over z, y), head: 4 (over x, core).
Axes of the slice: x: 2, y: 2, z: 4, core: 2. Of those that a mesh axis runs over, the one named last changes fastest.
Arguments:
- byte_input: float32 [3072, 2048], P('seq', 'head'), may hold values from -6 to 6
- b_proj: float32 [3072, 128], P('seq'), may hold values from -1.25 to 1.25
- c_proj: float32 [3072, 128], P('seq'), may hold values from -1.25 to 1.25
- step_decay: float32 [32, 3072], P('head', 'seq'), may hold values from 0 to 1
- skip_gain: float32 [32], P('head'), may hold values from 0.5 to 1.5
- out_weight: bfloat16 [2048, 1024], P('head'), may hold values from -0.125 to 0.125
- boundaries: int32 [8, 128], P('seq'), may hold values from 0 to 383, as said below
- counts: int32 [8], P('seq'), may hold values from 0 to 128, as said below
- norm_gain: float32 [1024], replicated, may hold values from 0.1 to 1.9
- qkv_weight: bfloat16 [3, 1024, 2048], P(None, None, 'head'), may hold values from -1 to 1
Outputs:
- attended: float32 [512, 2048], P('seq', 'head')
The draws below stay inside these ranges and needn't reach their ends.
Inputs may be any that keep to these rules, and one draw needn't show every extreme that they name: `boundaries`: row s holds counts[s] strictly increasing offsets, then zeros. The counts sum to 512; for every shard s the sum of the counts of shards before s lies within 32 of s * 64; some shard has 128.
All inputs are finite; a program needn't handle non-finite values.
Results may differ from the reference program's by a relative error of at most 0.0075.
Values may be sent and summed in bfloat16 or wider, within the bound.
A program may use at most 128 MiB of HBM per device.

```python
import jax
import jax.numpy as jnp
from jax import lax

D_ENC = 1024
RECURRENT_LANES = 32
STATE = 128
ATT_DIM = 64
BYTES_DEV = 384
ROWS_DEV = 64
D_INNER = 2048
D_MAIN = 2048
SLOTS = 128
SHARDS = 8
TOTAL_BYTES = 3072
COARSE = 512


def draw_step_decay(key, part):
    matched_entries = jax.random.split(jax.random.fold_in(key, 11), 7)
    share = 0.5
    fast = jax.random.uniform(matched_entries[0], (RECURRENT_LANES,)) < share
    fast_rate = jnp.exp(jax.random.uniform(matched_entries[1], (RECURRENT_LANES,), minval=jnp.log(1.0 / 50.0), maxval=jnp.log(1.0 / 30.0)))
    slow_rate = jax.random.uniform(matched_entries[2], (RECURRENT_LANES,), minval=0.3, maxval=0.6) / TOTAL_BYTES
    starting_shift = jnp.where(fast, fast_rate, slow_rate)
    partition_factor = jnp.exp(jax.random.uniform(matched_entries[3], (RECURRENT_LANES, SHARDS), minval=jnp.log(0.5), maxval=jnp.log(2.0)))
    partition_factor = jnp.repeat(partition_factor, BYTES_DEV, axis=1)
    approximate_guess = jax.random.uniform(matched_entries[4], (RECURRENT_LANES, TOTAL_BYTES), minval=0.5, maxval=1.5)
    destination_spots = jax.random.randint(matched_entries[5], (RECURRENT_LANES, 3), 0, TOTAL_BYTES)
    contiguous_extent = jax.random.uniform(matched_entries[6], (RECURRENT_LANES, 3), minval=0.22, maxval=0.69)
    entry_position = jnp.arange(TOTAL_BYTES)
    contiguous_bundles = jnp.sum(jnp.where(entry_position[None, None, :] == destination_spots[:, :, None], contiguous_extent[:, :, None], 0.0), axis=1)
    return (starting_shift[:, None] * partition_factor * approximate_guess + contiguous_bundles).astype(jnp.float32)


def boundary_plan(key):
    matched_entries = jax.random.split(jax.random.fold_in(key, 5), 3)
    half = ROWS_DEV // 2
    drift = jax.random.randint(matched_entries[0], (SHARDS,), -half, half + 1)
    summit = jax.random.randint(matched_entries[1], (), 1, SHARDS - 1)
    index = jnp.arange(SHARDS)
    drift = jnp.where(index == summit - 1, -half, drift)
    drift = jnp.where(index == summit, half, drift)
    drift = jnp.where(index == SHARDS - 1, 0, drift)
    before = jnp.concatenate([jnp.zeros((1,), drift.dtype), drift[:-1]])
    number = ROWS_DEV + drift - before
    orders = jax.vmap(lambda piece_key: jax.random.permutation(piece_key, BYTES_DEV))(jax.random.split(matched_entries[2], SHARDS))
    slot = jnp.arange(SLOTS)
    chosen = jnp.where(slot[None, :] < number[:, None], orders[:, :SLOTS], BYTES_DEV)
    chosen = jnp.sort(chosen, axis=1)
    chosen = jnp.where(slot[None, :] < number[:, None], chosen, 0)
    return (number.astype(jnp.int32), chosen.astype(jnp.int32))


def draw_counts(key, part):
    return boundary_plan(key)[0]


def draw_boundaries(key, part):
    return boundary_plan(key)[1]


def draw_qkv_weight(key, part):
    matched_entries = jax.random.split(jax.random.fold_in(key, 23), 1)
    spread = D_ENC ** (-0.5)
    drawn = jnp.clip(jax.random.normal(matched_entries[0], (3, D_ENC, D_MAIN)), -4.0, 4.0) * spread
    return jnp.clip(drawn, -1.0, 1.0).astype(jnp.bfloat16)


def block_levels(key, shape, cuts, least, top_value):
    factor_of, own = 1.0, jax.random.fold_in(key, 6)
    for dim, blocks in cuts:
        draws = jnp.exp(jax.random.uniform(jax.random.fold_in(own, dim), (blocks,), jnp.float32, least / len(cuts), top_value / len(cuts)))
        factor_of = factor_of * jnp.repeat(draws, shape[dim] // blocks).reshape([-1 if axis == dim else 1 for axis in range(len(shape))])
    return factor_of


def noise(key, dims, scale, reach, cuts=(), kind=jnp.bfloat16):
    values = scale * jax.random.normal(key, dims, jnp.float32)
    if cuts:
        values = values * block_levels(key, dims, cuts, -0.22, 0.18)
    return jnp.clip(values, -reach, reach).astype(kind)


def setup_inputs(seed: int = 0) -> dict:
    seeds = jax.random.split(jax.random.key(seed), 11)
    byte_input = noise(seeds[0], (TOTAL_BYTES, D_INNER), 1.0, 6.0, ((0, 8), (1, 4)), jnp.float32)
    b_proj = noise(seeds[1], (TOTAL_BYTES, STATE), (STATE ** -0.5), 1.25, ((0, 8),), jnp.float32)
    c_proj = noise(seeds[2], (TOTAL_BYTES, STATE), (STATE ** -0.5), 1.25, ((0, 8),), jnp.float32)
    step_decay = draw_step_decay(jax.random.fold_in(seeds[10], 71), 0)
    skip_gain = jnp.clip(0.5 + 1.0 * jax.random.uniform(seeds[4], (RECURRENT_LANES,), jnp.float32) ** block_levels(seeds[4], (RECURRENT_LANES,), ((0, 4),), -0.2, 0.2), 0.5, 1.5)
    out_weight = noise(seeds[5], (D_INNER, D_ENC), D_INNER ** -0.5, 0.125, ((0, 4),))
    boundaries = draw_boundaries(jax.random.fold_in(seeds[10], 71), 0)
    counts = draw_counts(jax.random.fold_in(seeds[10], 71), 0)
    norm_gain = jnp.clip(1.0 + 0.18 * jax.random.normal(seeds[8], (D_ENC,), jnp.float32), 0.1, 1.9)
    qkv_weight = draw_qkv_weight(jax.random.fold_in(seeds[10], 71), 0)
    return {"byte_input": byte_input, "b_proj": b_proj, "c_proj": c_proj, "step_decay": step_decay, "skip_gain": skip_gain, "out_weight": out_weight, "boundaries": boundaries, "counts": counts, "norm_gain": norm_gain, "qkv_weight": qkv_weight}


def state_space(inputs, b_rows, c_rows, decay):
    log_decay = jnp.cumsum(-decay, axis=1)
    affinity = jnp.dot(c_rows, b_rows.T, precision=lax.Precision.HIGHEST)
    length = inputs.shape[0]
    causal = lax.broadcasted_iota(jnp.int32, (length, length), 0) >= lax.broadcasted_iota(jnp.int32, (length, length), 1)

    def one_head(pair):
        values, logs = pair
        weights = jnp.where(causal, jnp.exp(jnp.where(causal, logs[:, None] - logs[None, :], 0.0)), 0.0) * affinity
        return jnp.dot(weights, values, precision=lax.Precision.HIGHEST)
    inside = lax.map(one_head, (inputs.transpose(1, 0, 2), log_decay))
    tail = jnp.exp(log_decay[:, -1:] - log_decay)
    own_state = jnp.einsum('ht,thp,tn->hpn', tail, inputs, b_rows, precision=lax.Precision.HIGHEST)
    return (log_decay, inside, own_state)

def reference(byte_input, b_proj, c_proj, step_decay, skip_gain, out_weight, boundaries, counts, norm_gain, qkv_weight):
    shards = counts.shape[0]
    heads = step_decay.shape[0]
    inputs = byte_input.reshape(shards, BYTES_DEV, heads, -1)
    b_rows = b_proj.reshape(shards, BYTES_DEV, -1)
    c_rows = c_proj.reshape(shards, BYTES_DEV, -1)
    decays = step_decay.reshape(heads, shards, BYTES_DEV).transpose(1, 0, 2)

    def advance(state, block):
        values, b_block, c_block, decay = block
        log_decay, inside, own_state = state_space(values, b_block, c_block, decay)
        carried = jnp.exp(log_decay)[:, :, None] * jnp.einsum('tn,hpn->htp', c_block, state, precision=lax.Precision.HIGHEST)
        mixed_heads = inside + carried + skip_gain[:, None, None] * values.transpose(1, 0, 2)
        new_state = jnp.exp(log_decay[:, -1])[:, None, None] * state + own_state
        return (new_state, mixed_heads)
    start_state = jnp.zeros((heads, inputs.shape[3], b_proj.shape[1]), jnp.float32)
    _, outputs = lax.scan(advance, start_state, (inputs, b_rows, c_rows, decays))
    y_rows = outputs.transpose(0, 2, 1, 3).reshape(shards * BYTES_DEV, -1).astype(jnp.bfloat16)
    slots = boundaries.shape[1]
    slot = jnp.arange(slots, dtype=jnp.int32)
    valid = slot[None, :] < counts[:, None]
    starts = (jnp.cumsum(counts) - counts).astype(jnp.int32)
    rank = jnp.where(valid, starts[:, None] + slot[None, :], COARSE).astype(jnp.int32)
    destination_spots = (boundaries + (jnp.arange(shards, dtype=jnp.int32) * BYTES_DEV)[:, None]).astype(jnp.int32)
    chosen = jnp.zeros((COARSE,), jnp.int32).at[rank.reshape(-1)].set(destination_spots.reshape(-1), mode='drop')
    rows = jnp.take(y_rows, chosen, axis=0)
    mixed = jnp.dot(rows, out_weight, preferred_element_type=jnp.float32)
    normed = (mixed * lax.rsqrt(lax.optimization_barrier(jnp.mean(mixed * mixed, axis=-1, keepdims=True)) + 1e-05) * norm_gain).astype(jnp.bfloat16)
    query = jnp.dot(normed, qkv_weight[0], preferred_element_type=jnp.float32).astype(jnp.bfloat16)
    keyed = jnp.dot(normed, qkv_weight[1], preferred_element_type=jnp.float32).astype(jnp.bfloat16)
    valued = jnp.dot(normed, qkv_weight[2], preferred_element_type=jnp.float32).astype(jnp.bfloat16)
    total = query.shape[0]
    causal = lax.broadcasted_iota(jnp.int32, (total, total), 0) >= lax.broadcasted_iota(jnp.int32, (total, total), 1)

    def split_heads(matrix):
        return matrix.reshape(total, -1, ATT_DIM).transpose(1, 0, 2)

    def attend(triple):
        q_head, k_head, v_head = triple
        scores = jnp.dot(q_head.astype(jnp.float32), k_head.astype(jnp.float32).T, precision=lax.Precision.HIGHEST) * ATT_DIM ** (-0.5)
        scores = jnp.where(causal, scores, -1e+30)
        highest = lax.optimization_barrier(jnp.max(scores, axis=-1, keepdims=True))
        exps = jnp.where(causal, jnp.exp(scores - highest), 0.0)
        sums = lax.optimization_barrier(jnp.sum(exps, axis=-1, keepdims=True))
        weights = exps.astype(jnp.bfloat16)
        return jnp.dot(weights, v_head, preferred_element_type=jnp.float32) / sums
    result = lax.map(attend, (split_heads(query), split_heads(keyed), split_heads(valued)))
    return result.transpose(1, 0, 2).reshape(total, -1)
```

```python
import functools

import jax
import jax.numpy as jnp
from jax import lax
from jax.experimental import pallas as pl
from jax.experimental.pallas import tpu as pltpu
from jax.sharding import PartitionSpec as P

ATT_DIM = 64
ROWS_DEV = 64


def prefix(shard, axis, combine, identity):
    length, here = (lax.axis_size(axis), lax.axis_index(axis))
    everything = jax.tree.map(lambda part: lax.all_gather(part, axis), shard)
    start = jax.tree.map(
        lambda part, zero: jnp.broadcast_to(jnp.asarray(zero, part.dtype), part.shape),
        shard,
        identity,
    )

    def lap(k, before):
        reached = k < here
        new = combine(before, jax.tree.map(lambda part: part[k], everything))
        return jax.tree.map(lambda a, b: jnp.where(reached, a, b), new, before)

    return lax.fori_loop(0, length, lap, start)


def extended(cells, sides, width):
    for axis, dim in sides:
        count = lax.axis_size(axis)
        ends = count - 1
        head = lax.slice_in_dim(cells, 0, width, axis=dim)
        tail = lax.slice_in_dim(cells, cells.shape[dim] - width, cells.shape[dim], axis=dim)
        cells = jnp.concatenate(
            [
                lax.ppermute(tail, axis, [(i, (i + 1) % count) for i in range(ends)]),
                cells,
                lax.ppermute(head, axis, [((i + 1) % count, i) for i in range(ends)]),
            ],
            axis=dim,
        )
    return cells


def state_space(inputs, b_rows, c_rows, decay):
    log_decay = jnp.cumsum(-decay, axis=1)
    affinity = jnp.dot(c_rows, b_rows.T, precision=lax.Precision.HIGHEST)
    length = inputs.shape[0]
    causal = lax.broadcasted_iota(jnp.int32, (length, length), 0) >= lax.broadcasted_iota(
        jnp.int32, (length, length), 1
    )

    def one_head(pair):
        values, logs = pair
        weights = (
            jnp.where(causal, jnp.exp(jnp.where(causal, logs[:, None] - logs[None, :], 0.0)), 0.0)
            * affinity
        )
        return jnp.dot(weights, values, precision=lax.Precision.HIGHEST)

    inside = lax.map(one_head, (inputs.transpose(1, 0, 2), log_decay))
    tail = jnp.exp(log_decay[:, -1:] - log_decay)
    own_state = jnp.einsum("ht,thp,tn->hpn", tail, inputs, b_rows, precision=lax.Precision.HIGHEST)
    return (log_decay, inside, own_state)


def link(earlier, later):
    return (earlier[0] * later[0], later[0][:, None, None] * earlier[1] + later[1])


def body(
    byte_input,
    b_proj,
    c_proj,
    step_decay,
    skip_gain,
    out_weight,
    boundaries,
    counts,
    norm_gain,
    qkv_weight,
):
    heads_here = step_decay.shape[0]
    length = byte_input.shape[0]
    inputs = byte_input.reshape(length, heads_here, -1)
    log_decay, inside, own_state = state_space(inputs, b_proj, c_proj, step_decay)
    span_decay = jnp.exp(log_decay[:, -1])
    arriving = prefix(
        (span_decay, own_state), "seq", link, (jnp.ones_like(span_decay), jnp.zeros_like(own_state))
    )
    carried = jnp.exp(log_decay)[:, :, None] * jnp.einsum(
        "tn,hpn->htp", c_proj, arriving[1], precision=lax.Precision.HIGHEST
    )
    mixed_heads = inside + carried + skip_gain[:, None, None] * inputs.transpose(1, 0, 2)
    slots = boundaries.shape[1]
    picked = jnp.take(mixed_heads, boundaries[0], axis=1)
    selected = picked.transpose(1, 0, 2).reshape(slots, -1).astype(jnp.bfloat16)
    all_counts = lax.all_gather(counts, "seq", axis=0, tiled=True)
    starts = jnp.cumsum(all_counts) - all_counts
    myself = lax.axis_index("seq")
    shards = lax.axis_size("seq")
    slot = jnp.arange(slots, dtype=jnp.int32)

    def slot_index(source):
        inside_axis = (source >= 0) & (source < shards)
        safe = jnp.clip(source, 0, shards - 1)
        begin = jnp.take(starts, safe)
        number = jnp.take(all_counts, safe)
        return jnp.where(inside_axis & (slot < number), begin + slot, -1)

    global_index = jnp.concatenate(
        [slot_index(myself - 1), slot_index(myself), slot_index(myself + 1)]
    )
    first_row = myself * ROWS_DEV
    target = first_row + jnp.arange(ROWS_DEV, dtype=jnp.int32)
    picker = global_index[None, :] == target[:, None]
    nearby = extended(selected, (("seq", 0),), slots)
    owned = jnp.dot(picker.astype(jnp.bfloat16), nearby, preferred_element_type=jnp.float32).astype(
        jnp.bfloat16
    )
    partial_value = jnp.dot(owned, out_weight, preferred_element_type=jnp.float32)
    packed = lax.psum(partial_value, "head")
    normed = (
        packed * lax.rsqrt(jnp.mean(packed * packed, axis=-1, keepdims=True) + 1e-05) * norm_gain
    ).astype(jnp.bfloat16)
    query = jnp.dot(normed, qkv_weight[0], preferred_element_type=jnp.float32).astype(jnp.bfloat16)
    keyed = jnp.dot(normed, qkv_weight[1], preferred_element_type=jnp.float32).astype(jnp.bfloat16)
    valued = jnp.dot(normed, qkv_weight[2], preferred_element_type=jnp.float32).astype(jnp.bfloat16)
    att_here = query.shape[1] // ATT_DIM
    queries = query.reshape(ROWS_DEV, att_here, ATT_DIM)
    row_place = first_row + jnp.arange(ROWS_DEV, dtype=jnp.int32)
    scale = ATT_DIM ** (-0.5)
    running = jnp.full((att_here, ROWS_DEV), -1e30, jnp.float32)
    key_piece = lax.all_gather(keyed, "seq", axis=0, tiled=True)
    value_piece = lax.all_gather(valued, "seq", axis=0, tiled=True)
    count = key_piece.shape[0]
    key_heads = key_piece.reshape(count, att_here, ATT_DIM)
    value_heads = value_piece.reshape(count, att_here, ATT_DIM)
    scores = (
        jnp.einsum("qhd,khd->hqk", queries, key_heads, preferred_element_type=jnp.float32) * scale
    )
    allowed = jnp.arange(count, dtype=jnp.int32)[None, :] <= row_place[:, None]
    scores = jnp.where(allowed[None], scores, -1e30)
    highest = jnp.maximum(running, jnp.max(scores, axis=-1))
    exps = jnp.where(allowed[None], jnp.exp(scores - highest[:, :, None]), 0.0)
    totals = jnp.sum(exps, axis=-1)
    weights = exps.astype(jnp.bfloat16)
    accum = jnp.einsum("hqk,khd->hqd", weights, value_heads, preferred_element_type=jnp.float32)
    running, totals, accum = (highest, totals, accum)
    result = accum / totals[:, :, None]
    return result.transpose(1, 0, 2).reshape(ROWS_DEV, att_here * ATT_DIM)


F32 = jnp.float32
BF16 = jnp.bfloat16
STATE_WIRE = jnp.float32
PART_WIRE = jnp.float32
EXTRA = 8


def exact_dot(a, b, dims=((1,), (0,))):
    return lax.dot_general(
        a, b, (dims, ((), ())), precision=lax.Precision.HIGHEST, preferred_element_type=F32
    )


def fast_dot(a, b, dims=((1,), (0,))):
    return lax.dot_general(a, b, (dims, ((), ())), preferred_element_type=F32)


def halves(a):
    high = a.astype(BF16)
    return high, (a - high.astype(F32)).astype(BF16)


def iota(shape, dim):
    return lax.broadcasted_iota(jnp.int32, shape, dim)


def fused(
    seqs,
    groups,
    counts_ref,
    skip_ref,
    x_ref,
    b_ref,
    c_ref,
    decay_ref,
    bound_ref,
    gain_ref,
    outw_hbm,
    qkvw_hbm,
    out_ref,
    outw,
    qkvw,
    send_a,
    recv_a,
    send_b,
    recv_b,
    send_p,
    recv_p,
    recv_n,
    send_q,
    recv_q,
    send_o,
    recv_o,
    weight_sem,
    a_sem,
    b_sem,
    p_send,
    p_recv,
    n_sem,
    q_sem,
    o_sem,
):
    me = lax.axis_index("seq")
    col = lax.axis_index("head")
    length, width = x_ref.shape
    heads = decay_ref.shape[0]
    lanes = width // heads
    state = b_ref.shape[1]
    slots = bound_ref.shape[1]
    rows = out_ref.shape[0]
    piece = rows // groups
    half = rows // 2

    outw_copy = pltpu.make_async_copy(outw_hbm, outw, weight_sem.at[0])
    qkvw_copy = pltpu.make_async_copy(qkvw_hbm, qkvw, weight_sem.at[1])
    outw_copy.start()
    qkvw_copy.start()

    def shard_at(d):
        return lax.rem(me + d + seqs, seqs)

    def head_at(d):
        return lax.rem(col + d, groups)

    barrier = pltpu.get_barrier_semaphore()
    peers = [(shard_at(d), col) for d in range(1, seqs)]
    peers += [(me, head_at(d)) for d in range(1, groups)]
    peers += [(shard_at(e), head_at(d)) for e in (-1, 1) for d in range(1, groups)]
    for peer in peers:
        pl.semaphore_signal(
            barrier, inc=1, device_id=peer, device_id_type=pl.DeviceIdType.MESH
        )

    def remote(src, dst, sems, k, peer):
        return pltpu.make_async_remote_copy(
            src_ref=src,
            dst_ref=dst,
            send_sem=sems.at[0, k],
            recv_sem=sems.at[1, k],
            device_id=peer,
            device_id_type=pl.DeviceIdType.MESH,
        )

    decay = decay_ref[...]
    upper = (iota((length, length), 0) <= iota((length, length), 1)).astype(F32)
    lower = (iota((length, length), 0) >= iota((length, length), 1)).astype(F32)
    logs = -exact_dot(decay, upper)
    logs_t = -exact_dot(lower, decay, ((1,), (1,)))
    first = iota((heads, width), 0) * lanes
    channel = iota((heads, width), 1)
    spread = ((channel >= first) & (channel < first + lanes)).astype(F32)
    tail_t = jnp.exp(logs_t[length - 1 : length, :] - logs_t)
    scaled = x_ref[...] * exact_dot(tail_t, spread)
    own = exact_dot(scaled, b_ref[...], ((0,), (0,)))
    number = jnp.full((EXTRA, state), counts_ref[0], jnp.int32).astype(F32)
    for h in range(heads):
        send_a[h, :lanes, :] = own[h * lanes : (h + 1) * lanes, :].astype(send_a.dtype)
        last = jnp.broadcast_to(logs[h : h + 1, length - 1 : length], (EXTRA, state))
        send_a[h, lanes:, :] = jnp.where(iota((EXTRA, state), 0) == 0, last, number)
    pl.semaphore_wait(barrier, len(peers))
    for d in range(1, seqs):
        to = shard_at(d)
        remote(send_a.at[to], recv_a.at[me], a_sem, d - 1, (to, col)).start()
    recv_a[me] = send_a[me]

    marks = jnp.broadcast_to(bound_ref[...].astype(F32), (slots, slots)).T
    marks = jnp.concatenate([marks] * (length // slots), axis=1)
    place = iota((slots, length), 1).astype(F32)
    hit = place == marks
    seen = place <= marks
    onehot = hit.astype(F32)
    c_rows = exact_dot(onehot, c_ref[...])
    logs_sel = exact_dot(onehot, logs_t)
    affinity = exact_dot(c_rows, b_ref[...], ((1,), (1,)))
    inside = []
    first_lane = iota((slots, 2 * lanes), 1) < lanes
    for pair in range(heads // 2):
        x_high, x_low = halves(x_ref[:, pair * 2 * lanes : (pair + 1) * 2 * lanes])
        x_both = jnp.concatenate([x_high, x_low], axis=1)
        parts = []
        for h in (2 * pair, 2 * pair + 1):
            gap = logs_sel[:, h : h + 1] - logs[h : h + 1, :]
            weights = jnp.where(seen, jnp.exp(jnp.where(seen, gap, 0.0)), 0.0) * affinity
            weights = weights + jnp.where(hit, skip_ref[h], 0.0)
            w_high, w_low = halves(weights)
            wide = fast_dot(w_high, x_both)
            parts.append(
                wide[:, : 2 * lanes] + wide[:, 2 * lanes :] + fast_dot(w_low, x_high)
            )
        inside.append(jnp.where(first_lane, parts[0], parts[1]))
    inside = jnp.concatenate(inside, axis=1)
    enter_scale = exact_dot(jnp.exp(logs_sel), spread)

    for d in range(1, seqs):
        source = shard_at(-d)
        copy = remote(send_a.at[shard_at(d)], recv_a.at[source], a_sem, d - 1, (source, col))
        copy.wait_recv()
    running = jnp.zeros((lanes, state), F32)
    for s in range(seqs):
        send_b[s] = running.astype(send_b.dtype)
        if s < seqs - 1:
            kept = jnp.exp(recv_a[s, lanes : lanes + 1, :])
            running = kept * running + recv_a[s, :lanes, :]
    for d in range(1, seqs):
        to = shard_at(d)
        remote(send_b.at[to], recv_b.at[me], b_sem, d - 1, (to, col)).start()
    recv_b[me] = send_b[me]

    start = jnp.zeros((1, state), F32)
    for s in range(seqs):
        start = start + jnp.where(s < me, recv_a[s, lanes + 1 : lanes + 2, :], 0.0)
    offset = start - (me * rows - half).astype(F32)
    slot = iota((slots, slots), 1).astype(F32)
    mine = jnp.full((slots, slots), counts_ref[0], jnp.int32).astype(F32)
    shift = (slot == iota((slots, slots), 0).astype(F32) - offset) & (slot < mine)
    shift = shift.astype(BF16)

    for d in range(1, seqs):
        source = shard_at(-d)
        remote(send_b.at[shard_at(d)], recv_b.at[source], b_sem, d - 1, (source, col)).wait_recv()
    entering = recv_b[...].reshape(heads * lanes, state).astype(F32)
    c_high, c_low = halves(c_rows)
    e_high, e_low = halves(entering)
    last_dims = ((1,), (1,))
    carried = (
        fast_dot(c_high, e_high, last_dims)
        + fast_dot(c_high, e_low, last_dims)
        + fast_dot(c_low, e_high, last_dims)
    )
    y = (inside + enter_scale * carried).astype(BF16)
    window = fast_dot(shift, y).astype(BF16)
    outw_copy.wait()
    partial = fast_dot(window, outw[...])
    pieces = slots // piece
    for i in range(pieces):
        send_p[i] = partial[i * piece : (i + 1) * piece, :].astype(send_p.dtype)
    outer = (pieces - groups) // 2

    def project(src, slot, k, peer):
        return pltpu.make_async_remote_copy(
            src_ref=send_p.at[src],
            dst_ref=recv_p.at[slot],
            send_sem=p_send.at[k],
            recv_sem=p_recv.at[slot],
            device_id=peer,
            device_id_type=pl.DeviceIdType.MESH,
        )

    sent = []
    for i in range(outer):
        sent.append(project(i, groups + col, i, (shard_at(-1), groups - outer + i)))
        sent.append(
            project(outer + groups + i, groups + col, outer + i, (shard_at(1), i))
        )
    for d in range(1, groups):
        to = head_at(d)
        sent.append(project(outer + to, col, 2 * outer + d - 1, (me, to)))
    for copy in sent:
        copy.start()
    recv_p[col] = send_p[outer + col]
    for d in range(1, groups):
        source = head_at(groups - d)
        project(0, source, 0, (me, source)).wait_recv()
    for k in range(groups):
        project(0, groups + k, 0, (shard_at(1), k)).wait_recv()
    mixed = recv_p[0].astype(F32)
    for k in range(1, 2 * groups):
        mixed = mixed + recv_p[k].astype(F32)
    square = jnp.mean(mixed * mixed, axis=-1, keepdims=True)
    normed = (mixed * lax.rsqrt(square + 1e-05) * gain_ref[...]).astype(BF16)
    recv_n[col] = normed
    sent_n = []
    for d in range(1, groups):
        to = head_at(d)
        sent_n.append(remote(recv_n.at[col], recv_n.at[col], n_sem, d - 1, (me, to)))
        sent_n[-1].start()
    for d in range(1, groups):
        source = head_at(groups - d)
        remote(recv_n.at[col], recv_n.at[source], n_sem, d - 1, (me, source)).wait_recv()
    normed = recv_n[...].reshape(rows, -1)
    qkvw_copy.wait()
    query, key, value = [
        fast_dot(normed, qkvw[i]).astype(BF16).astype(F32) for i in range(3)
    ]
    pair_width = 2 * lanes
    left = iota((rows, pair_width), 1) < lanes
    left_half = left[:half]

    def turned(a):
        return pltpu.roll(a, lanes, 1)

    for pair in range(heads // 2):
        at = slice(pair * pair_width, (pair + 1) * pair_width)
        q, k, v = query[:, at], key[:, at], value[:, at]
        send_q[2 * pair, :rows, :] = jnp.where(left, q, turned(k)).astype(BF16)
        send_q[2 * pair + 1, :rows, :] = jnp.where(left, turned(q), k).astype(BF16)
        above, below = v[:half], v[half:]
        send_q[2 * pair, rows:, :] = jnp.where(left_half, above, turned(below)).astype(BF16)
        send_q[2 * pair + 1, rows:, :] = jnp.where(
            left_half, turned(above), below
        ).astype(BF16)
    for d in range(1, seqs):
        to = shard_at(d)
        remote(send_q.at[to], recv_q.at[me], q_sem, d - 1, (to, col)).start()
    recv_q[me] = send_q[me]
    for d in range(1, seqs):
        source = shard_at(-d)
        remote(send_q.at[shard_at(d)], recv_q.at[source], q_sem, d - 1, (source, col)).wait_recv()
    coarse = seqs * rows
    both = recv_q[:, :rows, :].reshape(coarse, pair_width)
    wide = both.astype(F32)
    left_all = iota((coarse, pair_width), 1) < lanes
    queries = jnp.where(left_all, wide, 0.0).astype(BF16)
    keys = turned(wide).astype(BF16)
    values = []
    for s in range(seqs):
        packed = recv_q[s, rows:, :].astype(F32)
        values += [packed, turned(packed)]
    values = jnp.concatenate(values, axis=0).astype(BF16)
    scores = fast_dot(queries, keys, ((1,), (1,))) * (lanes ** (-0.5))
    allowed = iota((coarse, coarse), 0) >= iota((coarse, coarse), 1)
    scores = jnp.where(allowed, scores, -1e30)
    highest = jnp.max(scores, axis=-1, keepdims=True)
    exps = jnp.where(allowed, jnp.exp(scores - highest), 0.0)
    total = jnp.sum(exps, axis=-1, keepdims=True)
    result = fast_dot(exps.astype(BF16), values) / total
    for s in range(seqs):
        above = result[s * rows : s * rows + half]
        below = result[s * rows + half : (s + 1) * rows]
        send_o[s] = jnp.where(left_half, above, turned(below))
    for d in range(1, seqs):
        to = shard_at(d)
        remote(send_o.at[to], recv_o.at[me], o_sem, d - 1, (to, col)).start()
    recv_o[me] = send_o[me]
    for d in range(1, seqs):
        source = shard_at(-d)
        remote(send_o.at[shard_at(d)], recv_o.at[source], o_sem, d - 1, (source, col)).wait_recv()
    for pair in range(heads // 2):
        at = slice(pair * pair_width, (pair + 1) * pair_width)
        even, odd = recv_o[2 * pair], recv_o[2 * pair + 1]
        out_ref[:half, at] = jnp.where(left_half, even, turned(odd))
        out_ref[half:, at] = jnp.where(left_half, turned(even), odd)

    for copy in sent + sent_n:
        copy.wait_send()
    for sems, send, recv in (
        (a_sem, send_a, recv_a),
        (b_sem, send_b, recv_b),
        (q_sem, send_q, recv_q),
        (o_sem, send_o, recv_o),
    ):
        for d in range(1, seqs):
            to = shard_at(d)
            remote(send.at[to], recv.at[me], sems, d - 1, (to, col)).wait_send()


def fused_body(
    byte_input,
    b_proj,
    c_proj,
    step_decay,
    skip_gain,
    out_weight,
    boundaries,
    counts,
    norm_gain,
    qkv_weight,
):
    seqs, groups = lax.axis_size("seq"), lax.axis_size("head")
    heads = step_decay.shape[0]
    width = byte_input.shape[1]
    lanes = width // heads
    state = b_proj.shape[1]
    rows = ROWS_DEV
    piece = rows // groups
    enc = out_weight.shape[1]
    pieces = boundaries.shape[1] // piece
    vmem = pl.BlockSpec(memory_space=pltpu.VMEM)
    smem = pl.BlockSpec(memory_space=pltpu.SMEM)
    hbm = pl.BlockSpec(memory_space=pl.ANY)
    dma = pltpu.SemaphoreType.DMA
    return pl.pallas_call(
        functools.partial(fused, seqs, groups),
        out_shape=jax.ShapeDtypeStruct((rows, width), F32),
        in_specs=[smem, smem] + [vmem] * 6 + [hbm] * 2,
        out_specs=vmem,
        scratch_shapes=[
            pltpu.VMEM(out_weight.shape, BF16),
            pltpu.VMEM(qkv_weight.shape, BF16),
            pltpu.VMEM((seqs, lanes + EXTRA, state), STATE_WIRE),
            pltpu.VMEM((seqs, lanes + EXTRA, state), STATE_WIRE),
            pltpu.VMEM((seqs, lanes, state), STATE_WIRE),
            pltpu.VMEM((seqs, lanes, state), STATE_WIRE),
            pltpu.VMEM((pieces, piece, enc), PART_WIRE),
            pltpu.VMEM((2 * groups, piece, enc), PART_WIRE),
            pltpu.VMEM((groups, piece, enc), BF16),
            pltpu.VMEM((seqs, rows + rows // 2, 2 * lanes), BF16),
            pltpu.VMEM((seqs, rows + rows // 2, 2 * lanes), BF16),
            pltpu.VMEM((seqs, rows // 2, 2 * lanes), F32),
            pltpu.VMEM((seqs, rows // 2, 2 * lanes), F32),
            dma((2,)),
            dma((2, seqs - 1)),
            dma((2, seqs - 1)),
            dma((2 * groups,)),
            dma((2 * groups,)),
            dma((2, groups - 1)),
            dma((2, seqs - 1)),
            dma((2, seqs - 1)),
        ],
        compiler_params=pltpu.CompilerParams(collective_id=0, has_side_effects=True),
    )(
        counts,
        skip_gain,
        byte_input,
        b_proj,
        c_proj,
        step_decay,
        boundaries,
        norm_gain.reshape(1, -1),
        out_weight,
        qkv_weight,
    )


def chosen(*args):
    byte_input, step_decay, slots = args[0], args[3], args[6].shape[1]
    heads = step_decay.shape[0]
    lanes = byte_input.shape[1] // heads
    seqs, groups = lax.axis_size("seq"), lax.axis_size("head")
    fits = seqs == heads and lanes == ATT_DIM and args[9].shape[2] == byte_input.shape[1]
    fits = fits and 2 * lanes == slots and args[1].shape[1] == slots and slots == 2 * ROWS_DEV
    fits = fits and groups % 2 == 0 and ROWS_DEV % (16 * groups) == 0
    fits = fits and byte_input.shape[0] % slots == 0
    return fused_body(*args) if fits else body(*args)


def solution(mesh):
    return jax.shard_map(
        chosen,
        mesh=mesh,
        in_specs=(
            P("seq", "head"),
            P("seq", None),
            P("seq", None),
            P("head", "seq"),
            P("head"),
            P("head", None),
            P("seq", None),
            P("seq"),
            P(),
            P(None, None, "head"),
        ),
        out_specs=P("seq", "head"),
        check_vma=False,
    )
```

```python
import functools

import jax
import jax.numpy as jnp
from jax import lax
from jax.experimental import pallas as pl
from jax.experimental.pallas import tpu as pltpu
from jax.sharding import PartitionSpec as P

ATT_DIM = 64
ROWS_DEV = 64


def prefix(shard, axis, combine, identity):
    length, here = (lax.axis_size(axis), lax.axis_index(axis))
    everything = jax.tree.map(lambda part: lax.all_gather(part, axis), shard)
    start = jax.tree.map(
        lambda part, zero: jnp.broadcast_to(jnp.asarray(zero, part.dtype), part.shape),
        shard,
        identity,
    )

    def lap(k, before):
        reached = k < here
        new = combine(before, jax.tree.map(lambda part: part[k], everything))
        return jax.tree.map(lambda a, b: jnp.where(reached, a, b), new, before)

    return lax.fori_loop(0, length, lap, start)


def extended(cells, sides, width):
    for axis, dim in sides:
        count = lax.axis_size(axis)
        ends = count - 1
        head = lax.slice_in_dim(cells, 0, width, axis=dim)
        tail = lax.slice_in_dim(cells, cells.shape[dim] - width, cells.shape[dim], axis=dim)
        cells = jnp.concatenate(
            [
                lax.ppermute(tail, axis, [(i, (i + 1) % count) for i in range(ends)]),
                cells,
                lax.ppermute(head, axis, [((i + 1) % count, i) for i in range(ends)]),
            ],
            axis=dim,
        )
    return cells


def state_space(inputs, b_rows, c_rows, decay):
    log_decay = jnp.cumsum(-decay, axis=1)
    affinity = jnp.dot(c_rows, b_rows.T, precision=lax.Precision.HIGHEST)
    length = inputs.shape[0]
    causal = lax.broadcasted_iota(jnp.int32, (length, length), 0) >= lax.broadcasted_iota(
        jnp.int32, (length, length), 1
    )

    def one_head(pair):
        values, logs = pair
        weights = (
            jnp.where(causal, jnp.exp(jnp.where(causal, logs[:, None] - logs[None, :], 0.0)), 0.0)
            * affinity
        )
        return jnp.dot(weights, values, precision=lax.Precision.HIGHEST)

    inside = lax.map(one_head, (inputs.transpose(1, 0, 2), log_decay))
    tail = jnp.exp(log_decay[:, -1:] - log_decay)
    own_state = jnp.einsum("ht,thp,tn->hpn", tail, inputs, b_rows, precision=lax.Precision.HIGHEST)
    return (log_decay, inside, own_state)


def link(earlier, later):
    return (earlier[0] * later[0], later[0][:, None, None] * earlier[1] + later[1])


def body(
    byte_input,
    b_proj,
    c_proj,
    step_decay,
    skip_gain,
    out_weight,
    boundaries,
    counts,
    norm_gain,
    qkv_weight,
):
    heads_here = step_decay.shape[0]
    length = byte_input.shape[0]
    inputs = byte_input.reshape(length, heads_here, -1)
    log_decay, inside, own_state = state_space(inputs, b_proj, c_proj, step_decay)
    span_decay = jnp.exp(log_decay[:, -1])
    arriving = prefix(
        (span_decay, own_state), "seq", link, (jnp.ones_like(span_decay), jnp.zeros_like(own_state))
    )
    carried = jnp.exp(log_decay)[:, :, None] * jnp.einsum(
        "tn,hpn->htp", c_proj, arriving[1], precision=lax.Precision.HIGHEST
    )
    mixed_heads = inside + carried + skip_gain[:, None, None] * inputs.transpose(1, 0, 2)
    slots = boundaries.shape[1]
    picked = jnp.take(mixed_heads, boundaries[0], axis=1)
    selected = picked.transpose(1, 0, 2).reshape(slots, -1).astype(jnp.bfloat16)
    all_counts = lax.all_gather(counts, "seq", axis=0, tiled=True)
    starts = jnp.cumsum(all_counts) - all_counts
    myself = lax.axis_index("seq")
    shards = lax.axis_size("seq")
    slot = jnp.arange(slots, dtype=jnp.int32)

    def slot_index(source):
        inside_axis = (source >= 0) & (source < shards)
        safe = jnp.clip(source, 0, shards - 1)
        begin = jnp.take(starts, safe)
        number = jnp.take(all_counts, safe)
        return jnp.where(inside_axis & (slot < number), begin + slot, -1)

    global_index = jnp.concatenate(
        [slot_index(myself - 1), slot_index(myself), slot_index(myself + 1)]
    )
    first_row = myself * ROWS_DEV
    target = first_row + jnp.arange(ROWS_DEV, dtype=jnp.int32)
    picker = global_index[None, :] == target[:, None]
    nearby = extended(selected, (("seq", 0),), slots)
    owned = jnp.dot(picker.astype(jnp.bfloat16), nearby, preferred_element_type=jnp.float32).astype(
        jnp.bfloat16
    )
    partial_value = jnp.dot(owned, out_weight, preferred_element_type=jnp.float32)
    packed = lax.psum(partial_value, "head")
    normed = (
        packed * lax.rsqrt(jnp.mean(packed * packed, axis=-1, keepdims=True) + 1e-05) * norm_gain
    ).astype(jnp.bfloat16)
    query = jnp.dot(normed, qkv_weight[0], preferred_element_type=jnp.float32).astype(jnp.bfloat16)
    keyed = jnp.dot(normed, qkv_weight[1], preferred_element_type=jnp.float32).astype(jnp.bfloat16)
    valued = jnp.dot(normed, qkv_weight[2], preferred_element_type=jnp.float32).astype(jnp.bfloat16)
    att_here = query.shape[1] // ATT_DIM
    queries = query.reshape(ROWS_DEV, att_here, ATT_DIM)
    row_place = first_row + jnp.arange(ROWS_DEV, dtype=jnp.int32)
    scale = ATT_DIM ** (-0.5)
    running = jnp.full((att_here, ROWS_DEV), -1e30, jnp.float32)
    key_piece = lax.all_gather(keyed, "seq", axis=0, tiled=True)
    value_piece = lax.all_gather(valued, "seq", axis=0, tiled=True)
    count = key_piece.shape[0]
    key_heads = key_piece.reshape(count, att_here, ATT_DIM)
    value_heads = value_piece.reshape(count, att_here, ATT_DIM)
    scores = (
        jnp.einsum("qhd,khd->hqk", queries, key_heads, preferred_element_type=jnp.float32) * scale
    )
    allowed = jnp.arange(count, dtype=jnp.int32)[None, :] <= row_place[:, None]
    scores = jnp.where(allowed[None], scores, -1e30)
    highest = jnp.maximum(running, jnp.max(scores, axis=-1))
    exps = jnp.where(allowed[None], jnp.exp(scores - highest[:, :, None]), 0.0)
    totals = jnp.sum(exps, axis=-1)
    weights = exps.astype(jnp.bfloat16)
    accum = jnp.einsum("hqk,khd->hqd", weights, value_heads, preferred_element_type=jnp.float32)
    running, totals, accum = (highest, totals, accum)
    result = accum / totals[:, :, None]
    return result.transpose(1, 0, 2).reshape(ROWS_DEV, att_here * ATT_DIM)


F32 = jnp.float32
BF16 = jnp.bfloat16
STATE_WIRE = jnp.bfloat16
PART_WIRE = jnp.bfloat16
OUT_WIRE = jnp.bfloat16
EXTRA = 16


def exact_dot(a, b, dims=((1,), (0,))):
    return lax.dot_general(
        a, b, (dims, ((), ())), precision=lax.Precision.HIGHEST, preferred_element_type=F32
    )


def fast_dot(a, b, dims=((1,), (0,))):
    return lax.dot_general(a, b, (dims, ((), ())), preferred_element_type=F32)


def halves(a):
    high = a.astype(BF16)
    return high, (a - high.astype(F32)).astype(BF16)


def iota(shape, dim):
    return lax.broadcasted_iota(jnp.int32, shape, dim)


def fused(
    seqs,
    groups,
    decay_hbm,
    x_hbm,
    b_hbm,
    counts_hbm,
    bound_hbm,
    c_hbm,
    skip_hbm,
    outw_hbm,
    gain_hbm,
    qkvw_hbm,
    out_ref,
    decay_ref,
    x_ref,
    b_ref,
    counts_ref,
    bound_ref,
    c_ref,
    skip_ref,
    outw,
    gain_ref,
    qkvw,
    send_a,
    recv_a,
    send_b,
    recv_b,
    send_p,
    recv_p,
    recv_n,
    send_q,
    recv_q,
    send_o,
    recv_o,
    weight_sem,
    a_sem,
    b_sem,
    p_send,
    p_recv,
    n_sem,
    q_sem,
    o_sem,
):
    me = lax.axis_index("seq")
    col = lax.axis_index("head")
    length, width = x_ref.shape
    heads = decay_ref.shape[0]
    lanes = width // heads
    state = b_ref.shape[1]
    slots = bound_ref.shape[1]
    rows = out_ref.shape[0]
    piece = rows // groups
    half = rows // 2

    def shard_at(d):
        return lax.rem(me + d + seqs, seqs)

    def head_at(d):
        return lax.rem(col + d, groups)

    barrier = pltpu.get_barrier_semaphore()
    peers = [(shard_at(d), col) for d in range(1, seqs)]
    peers += [(me, head_at(d)) for d in range(1, groups)]
    peers += [(shard_at(e), head_at(d)) for e in (-1, 1) for d in range(1, groups)]
    for peer in peers:
        pl.semaphore_signal(
            barrier, inc=1, device_id=peer, device_id_type=pl.DeviceIdType.MESH
        )

    def remote(src, dst, sems, k, peer):
        return pltpu.make_async_remote_copy(
            src_ref=src,
            dst_ref=dst,
            send_sem=sems.at[0, k],
            recv_sem=sems.at[1, k],
            device_id=peer,
            device_id_type=pl.DeviceIdType.MESH,
        )

    loads = [
        pltpu.make_async_copy(source, target, weight_sem.at[i])
        for i, (source, target) in enumerate(
            (
                (decay_hbm, decay_ref),
                (x_hbm, x_ref),
                (b_hbm, b_ref),
                (counts_hbm, counts_ref),
                (bound_hbm, bound_ref),
                (c_hbm, c_ref),
                (skip_hbm, skip_ref),
                (outw_hbm, outw),
                (gain_hbm, gain_ref),
                (qkvw_hbm, qkvw),
            )
        )
    ]
    for load in loads:
        load.start()

    loads[0].wait()
    decay = decay_ref[...]
    upper = (iota((length, length), 0) <= iota((length, length), 1)).astype(F32)
    lower = (iota((length, length), 0) >= iota((length, length), 1)).astype(F32)
    logs = -exact_dot(decay, upper)
    logs_t = -exact_dot(lower, decay, ((1,), (1,)))
    first = iota((heads, width), 0) * lanes
    channel = iota((heads, width), 1)
    spread = ((channel >= first) & (channel < first + lanes)).astype(F32)
    tail_t = jnp.exp(logs_t[length - 1 : length, :] - logs_t)
    loads[1].wait()
    loads[2].wait()
    loads[3].wait()
    scaled = x_ref[...] * exact_dot(tail_t, spread)
    own = exact_dot(scaled, b_ref[...], ((0,), (0,)))
    number = jnp.broadcast_to(counts_ref[...].astype(F32), (EXTRA, state))
    extra_row = iota((EXTRA, state), 0)
    for h in range(heads):
        send_a[h, :lanes, :] = own[h * lanes : (h + 1) * lanes, :].astype(send_a.dtype)
        last = jnp.broadcast_to(logs[h : h + 1, length - 1 : length], (EXTRA, state))
        last_high, rest = halves(last)
        rest = last - last_high.astype(F32)
        last_mid, last_low = halves(rest)
        extra = jnp.where(extra_row == 1, last_mid.astype(F32), last_high.astype(F32))
        extra = jnp.where(extra_row == 2, last_low.astype(F32), extra)
        extra = jnp.where(extra_row == 3, number, extra)
        send_a[h, lanes:, :] = extra.astype(send_a.dtype)
    pl.semaphore_wait(barrier, len(peers))
    for d in range(1, seqs):
        to = shard_at(d)
        remote(send_a.at[to], recv_a.at[me], a_sem, d - 1, (to, col)).start()
    recv_a[me] = send_a[me]

    for load in loads[4:7]:
        load.wait()
    marks = jnp.broadcast_to(bound_ref[...].astype(F32), (slots, slots)).T
    marks = jnp.concatenate([marks] * (length // slots), axis=1)
    place = iota((slots, length), 1).astype(F32)
    hit = place == marks
    seen = place <= marks
    onehot = hit.astype(F32)
    c_rows = exact_dot(onehot, c_ref[...])
    logs_sel = exact_dot(onehot, logs_t)
    affinity = exact_dot(c_rows, b_ref[...], ((1,), (1,)))
    inside = []
    first_lane = iota((slots, 2 * lanes), 1) < lanes
    for pair in range(heads // 2):
        x_high, x_low = halves(x_ref[:, pair * 2 * lanes : (pair + 1) * 2 * lanes])
        x_both = jnp.concatenate([x_high, x_low], axis=1)
        parts = []
        for h in (2 * pair, 2 * pair + 1):
            gap = logs_sel[:, h : h + 1] - logs[h : h + 1, :]
            weights = jnp.where(seen, jnp.exp(jnp.where(seen, gap, 0.0)), 0.0) * affinity
            weights = weights + jnp.where(hit, skip_ref[:, h : h + 1], 0.0)
            w_high, w_low = halves(weights)
            wide = fast_dot(w_high, x_both)
            parts.append(
                wide[:, : 2 * lanes] + wide[:, 2 * lanes :] + fast_dot(w_low, x_high)
            )
        inside.append(jnp.where(first_lane, parts[0], parts[1]))
    inside = jnp.concatenate(inside, axis=1)
    enter_scale = exact_dot(jnp.exp(logs_sel), spread)

    for d in range(1, seqs):
        source = shard_at(-d)
        copy = remote(send_a.at[shard_at(d)], recv_a.at[source], a_sem, d - 1, (source, col))
        copy.wait_recv()
    running = jnp.zeros((lanes, state), F32)
    for s in range(seqs):
        send_b[s] = running.astype(send_b.dtype)
        if s < seqs - 1:
            tags = recv_a[s, lanes:, :].astype(F32)
            kept = jnp.exp((tags[0:1] + tags[1:2]) + tags[2:3])
            running = kept * running + recv_a[s, :lanes, :].astype(F32)
    for d in range(1, seqs):
        to = shard_at(d)
        remote(send_b.at[to], recv_b.at[me], b_sem, d - 1, (to, col)).start()
    recv_b[me] = send_b[me]

    start = jnp.zeros((1, state), F32)
    for s in range(seqs):
        start = start + jnp.where(s < me, recv_a[s, lanes:, :].astype(F32)[3:4], 0.0)
    offset = start - (me * rows - half).astype(F32)
    slot = iota((slots, slots), 1).astype(F32)
    mine = jnp.broadcast_to(counts_ref[...].astype(F32), (slots, slots))
    shift = (slot == iota((slots, slots), 0).astype(F32) - offset) & (slot < mine)
    shift = shift.astype(BF16)

    for d in range(1, seqs):
        source = shard_at(-d)
        remote(send_b.at[shard_at(d)], recv_b.at[source], b_sem, d - 1, (source, col)).wait_recv()
    entering = recv_b[...].reshape(heads * lanes, state)
    c_high, c_low = halves(c_rows)
    last_dims = ((1,), (1,))
    carried = fast_dot(c_high, entering, last_dims) + fast_dot(c_low, entering, last_dims)
    y = (inside + enter_scale * carried).astype(BF16)
    window = fast_dot(shift, y).astype(BF16)
    loads[7].wait()
    partial = fast_dot(window, outw[...])
    pieces = slots // piece
    for i in range(pieces):
        send_p[i] = partial[i * piece : (i + 1) * piece, :].astype(send_p.dtype)
    outer = (pieces - groups) // 2

    def project(src, slot, k, peer):
        return pltpu.make_async_remote_copy(
            src_ref=send_p.at[src],
            dst_ref=recv_p.at[slot],
            send_sem=p_send.at[k],
            recv_sem=p_recv.at[slot],
            device_id=peer,
            device_id_type=pl.DeviceIdType.MESH,
        )

    sent = []
    for i in range(outer):
        sent.append(project(i, groups + col, i, (shard_at(-1), groups - outer + i)))
        sent.append(
            project(outer + groups + i, groups + col, outer + i, (shard_at(1), i))
        )
    for d in range(1, groups):
        to = head_at(d)
        sent.append(project(outer + to, col, 2 * outer + d - 1, (me, to)))
    for copy in sent:
        copy.start()
    recv_p[col] = send_p[outer + col]
    for d in range(1, groups):
        source = head_at(groups - d)
        project(0, source, 0, (me, source)).wait_recv()
    for k in range(groups):
        project(0, groups + k, 0, (shard_at(1), k)).wait_recv()
    loads[8].wait()
    mixed = recv_p[0].astype(F32)
    for k in range(1, 2 * groups):
        mixed = mixed + recv_p[k].astype(F32)
    square = jnp.mean(mixed * mixed, axis=-1, keepdims=True)
    normed = (mixed * lax.rsqrt(square + 1e-05) * gain_ref[...]).astype(BF16)
    recv_n[col] = normed
    sent_n = []
    for d in range(1, groups):
        to = head_at(d)
        sent_n.append(remote(recv_n.at[col], recv_n.at[col], n_sem, d - 1, (me, to)))
        sent_n[-1].start()
    for d in range(1, groups):
        source = head_at(groups - d)
        remote(recv_n.at[col], recv_n.at[source], n_sem, d - 1, (me, source)).wait_recv()
    normed = recv_n[...].reshape(rows, -1)
    loads[9].wait()
    query, key, value = [
        fast_dot(normed, qkvw[i]).astype(BF16).astype(F32) for i in range(3)
    ]
    pair_width = 2 * lanes
    left = iota((rows, pair_width), 1) < lanes
    left_half = left[:half]

    def turned(a):
        return pltpu.roll(a, lanes, 1)

    for pair in range(heads // 2):
        at = slice(pair * pair_width, (pair + 1) * pair_width)
        q, k, v = query[:, at], key[:, at], value[:, at]
        send_q[2 * pair, :rows, :] = jnp.where(left, q, turned(k)).astype(BF16)
        send_q[2 * pair + 1, :rows, :] = jnp.where(left, turned(q), k).astype(BF16)
        above, below = v[:half], v[half:]
        send_q[2 * pair, rows:, :] = jnp.where(left_half, above, turned(below)).astype(BF16)
        send_q[2 * pair + 1, rows:, :] = jnp.where(
            left_half, turned(above), below
        ).astype(BF16)
    for d in range(1, seqs):
        to = shard_at(d)
        remote(send_q.at[to], recv_q.at[me], q_sem, d - 1, (to, col)).start()
    recv_q[me] = send_q[me]
    for d in range(1, seqs):
        source = shard_at(-d)
        remote(send_q.at[shard_at(d)], recv_q.at[source], q_sem, d - 1, (source, col)).wait_recv()
    coarse = seqs * rows
    both = recv_q[:, :rows, :].reshape(coarse, pair_width)
    wide = both.astype(F32)
    left_all = iota((coarse, pair_width), 1) < lanes
    queries = jnp.where(left_all, wide, 0.0).astype(BF16)
    keys = turned(wide).astype(BF16)
    values = []
    for s in range(seqs):
        packed = recv_q[s, rows:, :].astype(F32)
        values += [packed, turned(packed)]
    values = jnp.concatenate(values, axis=0).astype(BF16)
    scores = fast_dot(queries, keys, ((1,), (1,))) * (lanes ** (-0.5))
    allowed = iota((coarse, coarse), 0) >= iota((coarse, coarse), 1)
    scores = jnp.where(allowed, scores, -1e30)
    highest = jnp.max(scores, axis=-1, keepdims=True)
    exps = jnp.where(allowed, jnp.exp(scores - highest), 0.0)
    total = jnp.sum(exps, axis=-1, keepdims=True)
    result = fast_dot(exps.astype(BF16), values) / total
    for s in range(seqs):
        above = result[s * rows : s * rows + half]
        below = result[s * rows + half : (s + 1) * rows]
        send_o[s] = jnp.where(left_half, above, turned(below)).astype(send_o.dtype)
    for d in range(1, seqs):
        to = shard_at(d)
        remote(send_o.at[to], recv_o.at[me], o_sem, d - 1, (to, col)).start()
    recv_o[me] = send_o[me]
    for d in range(1, seqs):
        source = shard_at(-d)
        remote(send_o.at[shard_at(d)], recv_o.at[source], o_sem, d - 1, (source, col)).wait_recv()
    for pair in range(heads // 2):
        at = slice(pair * pair_width, (pair + 1) * pair_width)
        even, odd = recv_o[2 * pair].astype(F32), recv_o[2 * pair + 1].astype(F32)
        out_ref[:half, at] = jnp.where(left_half, even, turned(odd)).astype(OUT_WIRE)
        out_ref[half:, at] = jnp.where(left_half, turned(even), odd).astype(OUT_WIRE)

    for copy in sent + sent_n:
        copy.wait_send()
    for sems, send, recv in (
        (a_sem, send_a, recv_a),
        (b_sem, send_b, recv_b),
        (q_sem, send_q, recv_q),
        (o_sem, send_o, recv_o),
    ):
        for d in range(1, seqs):
            to = shard_at(d)
            remote(send.at[to], recv.at[me], sems, d - 1, (to, col)).wait_send()


def fused_body(
    byte_input,
    b_proj,
    c_proj,
    step_decay,
    skip_gain,
    out_weight,
    boundaries,
    counts,
    norm_gain,
    qkv_weight,
):
    seqs, groups = lax.axis_size("seq"), lax.axis_size("head")
    heads = step_decay.shape[0]
    width = byte_input.shape[1]
    lanes = width // heads
    state = b_proj.shape[1]
    rows = ROWS_DEV
    piece = rows // groups
    enc = out_weight.shape[1]
    pieces = boundaries.shape[1] // piece
    vmem = pl.BlockSpec(memory_space=pltpu.VMEM)
    hbm = pl.BlockSpec(memory_space=pl.ANY)
    dma = pltpu.SemaphoreType.DMA
    operands = (
        step_decay,
        byte_input,
        b_proj,
        counts.reshape(1, 1),
        boundaries,
        c_proj,
        skip_gain.reshape(1, -1),
        out_weight,
        norm_gain.reshape(1, -1),
        qkv_weight,
    )
    result = pl.pallas_call(
        functools.partial(fused, seqs, groups),
        out_shape=jax.ShapeDtypeStruct((rows, width), OUT_WIRE),
        in_specs=[hbm] * len(operands),
        out_specs=vmem,
        scratch_shapes=[pltpu.VMEM(array.shape, array.dtype) for array in operands]
        + [
            pltpu.VMEM((seqs, lanes + EXTRA, state), STATE_WIRE),
            pltpu.VMEM((seqs, lanes + EXTRA, state), STATE_WIRE),
            pltpu.VMEM((seqs, lanes, state), STATE_WIRE),
            pltpu.VMEM((seqs, lanes, state), STATE_WIRE),
            pltpu.VMEM((pieces, piece, enc), PART_WIRE),
            pltpu.VMEM((2 * groups, piece, enc), PART_WIRE),
            pltpu.VMEM((groups, piece, enc), BF16),
            pltpu.VMEM((seqs, rows + rows // 2, 2 * lanes), BF16),
            pltpu.VMEM((seqs, rows + rows // 2, 2 * lanes), BF16),
            pltpu.VMEM((seqs, rows // 2, 2 * lanes), OUT_WIRE),
            pltpu.VMEM((seqs, rows // 2, 2 * lanes), OUT_WIRE),
            dma((len(operands),)),
            dma((2, seqs - 1)),
            dma((2, seqs - 1)),
            dma((2 * groups,)),
            dma((2 * groups,)),
            dma((2, groups - 1)),
            dma((2, seqs - 1)),
            dma((2, seqs - 1)),
        ],
        compiler_params=pltpu.CompilerParams(collective_id=0, has_side_effects=True),
    )(*operands)
    return result.astype(F32)


def chosen(*args):
    byte_input, step_decay, slots = args[0], args[3], args[6].shape[1]
    heads = step_decay.shape[0]
    lanes = byte_input.shape[1] // heads
    seqs, groups = lax.axis_size("seq"), lax.axis_size("head")
    fits = seqs == heads and lanes == ATT_DIM and args[9].shape[2] == byte_input.shape[1]
    fits = fits and 2 * lanes == slots and args[1].shape[1] == slots and slots == 2 * ROWS_DEV
    fits = fits and groups % 2 == 0 and ROWS_DEV % (16 * groups) == 0
    fits = fits and byte_input.shape[0] % slots == 0
    return fused_body(*args) if fits else body(*args)


def solution(mesh):
    return jax.shard_map(
        chosen,
        mesh=mesh,
        in_specs=(
            P("seq", "head"),
            P("seq", None),
            P("seq", None),
            P("head", "seq"),
            P("head"),
            P("head", None),
            P("seq", None),
            P("seq"),
            P(),
            P(None, None, "head"),
        ),
        out_specs=P("seq", "head"),
        check_vma=False,
    )
```

```python
import functools

import jax
import jax.numpy as jnp
from jax import lax
from jax.experimental import pallas as pl
from jax.experimental.pallas import tpu as pltpu
from jax.sharding import PartitionSpec as P

ATT_DIM = 64
ROWS_DEV = 64


def prefix(shard, axis, combine, identity):
    length, here = (lax.axis_size(axis), lax.axis_index(axis))
    everything = jax.tree.map(lambda part: lax.all_gather(part, axis), shard)
    start = jax.tree.map(
        lambda part, zero: jnp.broadcast_to(jnp.asarray(zero, part.dtype), part.shape),
        shard,
        identity,
    )

    def lap(k, before):
        reached = k < here
        new = combine(before, jax.tree.map(lambda part: part[k], everything))
        return jax.tree.map(lambda a, b: jnp.where(reached, a, b), new, before)

    return lax.fori_loop(0, length, lap, start)


def extended(cells, sides, width):
    for axis, dim in sides:
        count = lax.axis_size(axis)
        ends = count - 1
        head = lax.slice_in_dim(cells, 0, width, axis=dim)
        tail = lax.slice_in_dim(cells, cells.shape[dim] - width, cells.shape[dim], axis=dim)
        cells = jnp.concatenate(
            [
                lax.ppermute(tail, axis, [(i, (i + 1) % count) for i in range(ends)]),
                cells,
                lax.ppermute(head, axis, [((i + 1) % count, i) for i in range(ends)]),
            ],
            axis=dim,
        )
    return cells


def state_space(inputs, b_rows, c_rows, decay):
    log_decay = jnp.cumsum(-decay, axis=1)
    affinity = jnp.dot(c_rows, b_rows.T, precision=lax.Precision.HIGHEST)
    length = inputs.shape[0]
    causal = lax.broadcasted_iota(jnp.int32, (length, length), 0) >= lax.broadcasted_iota(
        jnp.int32, (length, length), 1
    )

    def one_head(pair):
        values, logs = pair
        weights = (
            jnp.where(causal, jnp.exp(jnp.where(causal, logs[:, None] - logs[None, :], 0.0)), 0.0)
            * affinity
        )
        return jnp.dot(weights, values, precision=lax.Precision.HIGHEST)

    inside = lax.map(one_head, (inputs.transpose(1, 0, 2), log_decay))
    tail = jnp.exp(log_decay[:, -1:] - log_decay)
    own_state = jnp.einsum("ht,thp,tn->hpn", tail, inputs, b_rows, precision=lax.Precision.HIGHEST)
    return (log_decay, inside, own_state)


def link(earlier, later):
    return (earlier[0] * later[0], later[0][:, None, None] * earlier[1] + later[1])


def body(
    byte_input,
    b_proj,
    c_proj,
    step_decay,
    skip_gain,
    out_weight,
    boundaries,
    counts,
    norm_gain,
    qkv_weight,
):
    heads_here = step_decay.shape[0]
    length = byte_input.shape[0]
    inputs = byte_input.reshape(length, heads_here, -1)
    log_decay, inside, own_state = state_space(inputs, b_proj, c_proj, step_decay)
    span_decay = jnp.exp(log_decay[:, -1])
    arriving = prefix(
        (span_decay, own_state), "seq", link, (jnp.ones_like(span_decay), jnp.zeros_like(own_state))
    )
    carried = jnp.exp(log_decay)[:, :, None] * jnp.einsum(
        "tn,hpn->htp", c_proj, arriving[1], precision=lax.Precision.HIGHEST
    )
    mixed_heads = inside + carried + skip_gain[:, None, None] * inputs.transpose(1, 0, 2)
    slots = boundaries.shape[1]
    picked = jnp.take(mixed_heads, boundaries[0], axis=1)
    selected = picked.transpose(1, 0, 2).reshape(slots, -1).astype(jnp.bfloat16)
    all_counts = lax.all_gather(counts, "seq", axis=0, tiled=True)
    starts = jnp.cumsum(all_counts) - all_counts
    myself = lax.axis_index("seq")
    shards = lax.axis_size("seq")
    slot = jnp.arange(slots, dtype=jnp.int32)

    def slot_index(source):
        inside_axis = (source >= 0) & (source < shards)
        safe = jnp.clip(source, 0, shards - 1)
        begin = jnp.take(starts, safe)
        number = jnp.take(all_counts, safe)
        return jnp.where(inside_axis & (slot < number), begin + slot, -1)

    global_index = jnp.concatenate(
        [slot_index(myself - 1), slot_index(myself), slot_index(myself + 1)]
    )
    first_row = myself * ROWS_DEV
    target = first_row + jnp.arange(ROWS_DEV, dtype=jnp.int32)
    picker = global_index[None, :] == target[:, None]
    nearby = extended(selected, (("seq", 0),), slots)
    owned = jnp.dot(picker.astype(jnp.bfloat16), nearby, preferred_element_type=jnp.float32).astype(
        jnp.bfloat16
    )
    partial_value = jnp.dot(owned, out_weight, preferred_element_type=jnp.float32)
    packed = lax.psum(partial_value, "head")
    normed = (
        packed * lax.rsqrt(jnp.mean(packed * packed, axis=-1, keepdims=True) + 1e-05) * norm_gain
    ).astype(jnp.bfloat16)
    query = jnp.dot(normed, qkv_weight[0], preferred_element_type=jnp.float32).astype(jnp.bfloat16)
    keyed = jnp.dot(normed, qkv_weight[1], preferred_element_type=jnp.float32).astype(jnp.bfloat16)
    valued = jnp.dot(normed, qkv_weight[2], preferred_element_type=jnp.float32).astype(jnp.bfloat16)
    att_here = query.shape[1] // ATT_DIM
    queries = query.reshape(ROWS_DEV, att_here, ATT_DIM)
    row_place = first_row + jnp.arange(ROWS_DEV, dtype=jnp.int32)
    scale = ATT_DIM ** (-0.5)
    running = jnp.full((att_here, ROWS_DEV), -1e30, jnp.float32)
    key_piece = lax.all_gather(keyed, "seq", axis=0, tiled=True)
    value_piece = lax.all_gather(valued, "seq", axis=0, tiled=True)
    count = key_piece.shape[0]
    key_heads = key_piece.reshape(count, att_here, ATT_DIM)
    value_heads = value_piece.reshape(count, att_here, ATT_DIM)
    scores = (
        jnp.einsum("qhd,khd->hqk", queries, key_heads, preferred_element_type=jnp.float32) * scale
    )
    allowed = jnp.arange(count, dtype=jnp.int32)[None, :] <= row_place[:, None]
    scores = jnp.where(allowed[None], scores, -1e30)
    highest = jnp.maximum(running, jnp.max(scores, axis=-1))
    exps = jnp.where(allowed[None], jnp.exp(scores - highest[:, :, None]), 0.0)
    totals = jnp.sum(exps, axis=-1)
    weights = exps.astype(jnp.bfloat16)
    accum = jnp.einsum("hqk,khd->hqd", weights, value_heads, preferred_element_type=jnp.float32)
    running, totals, accum = (highest, totals, accum)
    result = accum / totals[:, :, None]
    return result.transpose(1, 0, 2).reshape(ROWS_DEV, att_here * ATT_DIM)


F32 = jnp.float32
BF16 = jnp.bfloat16
STATE_WIRE = jnp.bfloat16
PART_WIRE = jnp.bfloat16
OUT_WIRE = jnp.bfloat16
EXTRA = 16


def exact_dot(a, b, dims=((1,), (0,))):
    return lax.dot_general(
        a, b, (dims, ((), ())), precision=lax.Precision.HIGHEST, preferred_element_type=F32
    )


def fast_dot(a, b, dims=((1,), (0,))):
    return lax.dot_general(a, b, (dims, ((), ())), preferred_element_type=F32)


def halves(a):
    high = a.astype(BF16)
    return high, (a - high.astype(F32)).astype(BF16)


def iota(shape, dim):
    return lax.broadcasted_iota(jnp.int32, shape, dim)


def fused(
    seqs,
    groups,
    decay_hbm,
    x_hbm,
    b_hbm,
    counts_hbm,
    bound_hbm,
    c_hbm,
    skip_hbm,
    outw_hbm,
    gain_hbm,
    qkvw_hbm,
    out_ref,
    decay_ref,
    x_ref,
    b_ref,
    counts_ref,
    bound_ref,
    c_ref,
    skip_ref,
    outw,
    gain_ref,
    qkvw,
    send_a,
    recv_a,
    send_b,
    recv_b,
    send_p,
    recv_p,
    recv_n,
    send_q,
    recv_q,
    send_o,
    recv_o,
    weight_sem,
    a_sem,
    b_sem,
    p_send,
    p_recv,
    n_sem,
    q_sem,
    o_sem,
):
    me = lax.axis_index("seq")
    col = lax.axis_index("head")
    length, width = x_ref.shape
    heads = decay_ref.shape[0]
    lanes = width // heads
    state = b_ref.shape[1]
    slots = bound_ref.shape[1]
    rows = out_ref.shape[0]
    piece = rows // groups
    half = rows // 2

    def shard_at(d):
        return lax.rem(me + d + seqs, seqs)

    layers = seqs // 2
    mid = layers // 2
    layer, side = me // 2, lax.rem(me, 2)
    near_end = layer < mid
    far_layers = [jnp.where(near_end, layers - 1 - k, k) for k in range(layers - mid)]
    same = jnp.where(near_end, layer, layer - (layers - mid))
    for k in range(1, mid):
        turn = lax.rem(same + k, mid)
        far_layers.append(jnp.where(near_end, turn, turn + (layers - mid)))
    targets = []
    for there in far_layers + [layer]:
        targets.append(2 * there + 1 - side)
        if there is not layer:
            targets.append(2 * there + side)

    def head_at(d):
        return lax.rem(col + d, groups)

    barrier = pltpu.get_barrier_semaphore()
    peers = [(shard_at(d), col) for d in range(1, seqs)]
    peers += [(me, head_at(d)) for d in range(1, groups)]
    peers += [(shard_at(e), head_at(d)) for e in (-1, 1) for d in range(1, groups)]
    for peer in peers:
        pl.semaphore_signal(
            barrier, inc=1, device_id=peer, device_id_type=pl.DeviceIdType.MESH
        )

    def remote(src, dst, sems, k, source, peer):
        return pltpu.make_async_remote_copy(
            src_ref=src,
            dst_ref=dst,
            send_sem=sems.at[0, k],
            recv_sem=sems.at[1, source],
            device_id=peer,
            device_id_type=pl.DeviceIdType.MESH,
        )

    loads = [
        pltpu.make_async_copy(source, target, weight_sem.at[i])
        for i, (source, target) in enumerate(
            (
                (decay_hbm, decay_ref),
                (x_hbm, x_ref),
                (b_hbm, b_ref),
                (counts_hbm, counts_ref),
                (bound_hbm, bound_ref),
                (c_hbm, c_ref),
                (skip_hbm, skip_ref),
                (outw_hbm, outw),
                (gain_hbm, gain_ref),
                (qkvw_hbm, qkvw),
            )
        )
    ]
    for load in loads:
        load.start()

    loads[0].wait()
    decay = decay_ref[...]
    upper = (iota((length, length), 0) <= iota((length, length), 1)).astype(F32)
    lower = (iota((length, length), 0) >= iota((length, length), 1)).astype(F32)
    logs = -exact_dot(decay, upper)
    logs_t = -exact_dot(lower, decay, ((1,), (1,)))
    first = iota((heads, width), 0) * lanes
    channel = iota((heads, width), 1)
    spread = ((channel >= first) & (channel < first + lanes)).astype(F32)
    tail_t = jnp.exp(logs_t[length - 1 : length, :] - logs_t)
    loads[1].wait()
    loads[2].wait()
    loads[3].wait()
    scaled = x_ref[...] * exact_dot(tail_t, spread)
    own = exact_dot(scaled, b_ref[...], ((0,), (0,)))
    number = jnp.broadcast_to(counts_ref[...].astype(F32), (EXTRA, state))
    extra_row = iota((EXTRA, state), 0)
    for h in range(heads):
        send_a[h, :lanes, :] = own[h * lanes : (h + 1) * lanes, :].astype(send_a.dtype)
        last = jnp.broadcast_to(logs[h : h + 1, length - 1 : length], (EXTRA, state))
        last_high, rest = halves(last)
        rest = last - last_high.astype(F32)
        last_mid, last_low = halves(rest)
        extra = jnp.where(extra_row == 1, last_mid.astype(F32), last_high.astype(F32))
        extra = jnp.where(extra_row == 2, last_low.astype(F32), extra)
        extra = jnp.where(extra_row == 3, number, extra)
        send_a[h, lanes:, :] = extra.astype(send_a.dtype)
    pl.semaphore_wait(barrier, len(peers))
    for to in targets:
        remote(send_a.at[to], recv_a.at[me], a_sem, to, me, (to, col)).start()
    recv_a[me] = send_a[me]

    for load in loads[4:7]:
        load.wait()
    marks = jnp.broadcast_to(bound_ref[...].astype(F32), (slots, slots)).T
    marks = jnp.concatenate([marks] * (length // slots), axis=1)
    place = iota((slots, length), 1).astype(F32)
    hit = place == marks
    seen = place <= marks
    onehot = hit.astype(F32)
    c_rows = exact_dot(onehot, c_ref[...])
    logs_sel = exact_dot(onehot, logs_t)
    affinity = exact_dot(c_rows, b_ref[...], ((1,), (1,)))
    inside = []
    first_lane = iota((slots, 2 * lanes), 1) < lanes
    for pair in range(heads // 2):
        x_high, x_low = halves(x_ref[:, pair * 2 * lanes : (pair + 1) * 2 * lanes])
        x_both = jnp.concatenate([x_high, x_low], axis=1)
        parts = []
        for h in (2 * pair, 2 * pair + 1):
            gap = logs_sel[:, h : h + 1] - logs[h : h + 1, :]
            weights = jnp.where(seen, jnp.exp(jnp.where(seen, gap, 0.0)), 0.0) * affinity
            weights = weights + jnp.where(hit, skip_ref[:, h : h + 1], 0.0)
            w_high, w_low = halves(weights)
            wide = fast_dot(w_high, x_both)
            parts.append(
                wide[:, : 2 * lanes] + wide[:, 2 * lanes :] + fast_dot(w_low, x_high)
            )
        inside.append(jnp.where(first_lane, parts[0], parts[1]))
    inside = jnp.concatenate(inside, axis=1)
    enter_scale = exact_dot(jnp.exp(logs_sel), spread)

    for d in range(1, seqs):
        source = shard_at(-d)
        copy = remote(send_a.at[shard_at(d)], recv_a.at[source], a_sem, source, source, (source, col))
        copy.wait_recv()
    running = jnp.zeros((lanes, state), F32)
    for s in range(seqs):
        send_b[s] = running.astype(send_b.dtype)
        if s < seqs - 1:
            tags = recv_a[s, lanes:, :].astype(F32)
            kept = jnp.exp((tags[0:1] + tags[1:2]) + tags[2:3])
            running = kept * running + recv_a[s, :lanes, :].astype(F32)
    for to in targets:
        remote(send_b.at[to], recv_b.at[me], b_sem, to, me, (to, col)).start()
    recv_b[me] = send_b[me]

    start = jnp.zeros((1, state), F32)
    for s in range(seqs):
        start = start + jnp.where(s < me, recv_a[s, lanes:, :].astype(F32)[3:4], 0.0)
    offset = start - (me * rows - half).astype(F32)
    slot = iota((slots, slots), 1).astype(F32)
    mine = jnp.broadcast_to(counts_ref[...].astype(F32), (slots, slots))
    shift = (slot == iota((slots, slots), 0).astype(F32) - offset) & (slot < mine)
    shift = shift.astype(BF16)

    for d in range(1, seqs):
        source = shard_at(-d)
        remote(send_b.at[shard_at(d)], recv_b.at[source], b_sem, source, source, (source, col)).wait_recv()
    entering = recv_b[...].reshape(heads * lanes, state)
    c_high, c_low = halves(c_rows)
    last_dims = ((1,), (1,))
    carried = fast_dot(c_high, entering, last_dims) + fast_dot(c_low, entering, last_dims)
    y = (inside + enter_scale * carried).astype(BF16)
    window = fast_dot(shift, y).astype(BF16)
    loads[7].wait()
    partial = fast_dot(window, outw[...])
    pieces = slots // piece
    for i in range(pieces):
        send_p[i] = partial[i * piece : (i + 1) * piece, :].astype(send_p.dtype)
    outer = (pieces - groups) // 2

    def project(src, slot, k, peer):
        return pltpu.make_async_remote_copy(
            src_ref=send_p.at[src],
            dst_ref=recv_p.at[slot],
            send_sem=p_send.at[k],
            recv_sem=p_recv.at[slot],
            device_id=peer,
            device_id_type=pl.DeviceIdType.MESH,
        )

    below_sent = [project(i, groups + col, i, (shard_at(-1), groups - outer + i)) for i in range(outer)]
    above_sent = [
        project(outer + groups + i, groups + col, outer + i, (shard_at(1), i))
        for i in range(outer)
    ]
    sent = []
    for d in range(1, groups):
        to = head_at(d)
        sent.append(project(outer + to, col, 2 * outer + d - 1, (me, to)))
    has_below, has_above = me > 0, me < seqs - 1

    @pl.when(has_below)
    def _():
        for copy in below_sent:
            copy.start()

    @pl.when(has_above)
    def _():
        for copy in above_sent:
            copy.start()

    for copy in sent:
        copy.start()
    recv_p[col] = send_p[outer + col]
    expects = (has_below & (col < outer)) | (has_above & (col >= outer))

    @pl.when(expects)
    def _():
        for k in range(groups):
            project(0, groups + k, 0, (shard_at(1), k)).wait_recv()

    @pl.when(jnp.logical_not(expects))
    def _():
        recv_p[groups:] = jnp.zeros((groups, piece, recv_p.shape[2]), recv_p.dtype)

    for d in range(1, groups):
        source = head_at(groups - d)
        project(0, source, 0, (me, source)).wait_recv()
    loads[8].wait()
    mixed = recv_p[0].astype(F32)
    for k in range(1, 2 * groups):
        mixed = mixed + recv_p[k].astype(F32)
    square = jnp.mean(mixed * mixed, axis=-1, keepdims=True)
    normed = (mixed * lax.rsqrt(square + 1e-05) * gain_ref[...]).astype(BF16)
    recv_n[col] = normed
    sent_n = []
    for d in range(1, groups):
        to = head_at(d)
        sent_n.append(remote(recv_n.at[col], recv_n.at[col], n_sem, to, col, (me, to)))
        sent_n[-1].start()
    for d in range(1, groups):
        source = head_at(groups - d)
        remote(recv_n.at[col], recv_n.at[source], n_sem, source, source, (me, source)).wait_recv()
    normed = recv_n[...].reshape(rows, -1)
    loads[9].wait()
    query, key, value = [
        fast_dot(normed, qkvw[i]).astype(BF16).astype(F32) for i in range(3)
    ]
    pair_width = 2 * lanes
    left = iota((rows, pair_width), 1) < lanes
    left_half = left[:half]

    def turned(a):
        return pltpu.roll(a, lanes, 1)

    for pair in range(heads // 2):
        at = slice(pair * pair_width, (pair + 1) * pair_width)
        q, k, v = query[:, at], key[:, at], value[:, at]
        send_q[2 * pair, :rows, :] = jnp.where(left, q, turned(k)).astype(BF16)
        send_q[2 * pair + 1, :rows, :] = jnp.where(left, turned(q), k).astype(BF16)
        above, below = v[:half], v[half:]
        send_q[2 * pair, rows:, :] = jnp.where(left_half, above, turned(below)).astype(BF16)
        send_q[2 * pair + 1, rows:, :] = jnp.where(
            left_half, turned(above), below
        ).astype(BF16)
    for to in targets:
        remote(send_q.at[to], recv_q.at[me], q_sem, to, me, (to, col)).start()
    recv_q[me] = send_q[me]
    for d in range(1, seqs):
        source = shard_at(-d)
        remote(send_q.at[shard_at(d)], recv_q.at[source], q_sem, source, source, (source, col)).wait_recv()
    coarse = seqs * rows
    both = recv_q[:, :rows, :].reshape(coarse, pair_width)
    wide = both.astype(F32)
    left_all = iota((coarse, pair_width), 1) < lanes
    queries = jnp.where(left_all, wide, 0.0).astype(BF16)
    keys = turned(wide).astype(BF16)
    values = []
    for s in range(seqs):
        packed = recv_q[s, rows:, :].astype(F32)
        values += [packed, turned(packed)]
    values = jnp.concatenate(values, axis=0).astype(BF16)
    scores = fast_dot(queries, keys, ((1,), (1,))) * (lanes ** (-0.5))
    allowed = iota((coarse, coarse), 0) >= iota((coarse, coarse), 1)
    scores = jnp.where(allowed, scores, -1e30)
    highest = jnp.max(scores, axis=-1, keepdims=True)
    exps = jnp.where(allowed, jnp.exp(scores - highest), 0.0)
    total = jnp.sum(exps, axis=-1, keepdims=True)
    result = fast_dot(exps.astype(BF16), values) / total
    for s in range(seqs):
        above = result[s * rows : s * rows + half]
        below = result[s * rows + half : (s + 1) * rows]
        send_o[s] = jnp.where(left_half, above, turned(below)).astype(send_o.dtype)
    for to in targets:
        remote(send_o.at[to], recv_o.at[me], o_sem, to, me, (to, col)).start()
    recv_o[me] = send_o[me]
    for d in range(1, seqs):
        source = shard_at(-d)
        remote(send_o.at[shard_at(d)], recv_o.at[source], o_sem, source, source, (source, col)).wait_recv()
    for pair in range(heads // 2):
        at = slice(pair * pair_width, (pair + 1) * pair_width)
        even, odd = recv_o[2 * pair].astype(F32), recv_o[2 * pair + 1].astype(F32)
        out_ref[:half, at] = jnp.where(left_half, even, turned(odd)).astype(OUT_WIRE)
        out_ref[half:, at] = jnp.where(left_half, turned(even), odd).astype(OUT_WIRE)

    for copy in sent + sent_n:
        copy.wait_send()

    @pl.when(has_below)
    def _():
        for copy in below_sent:
            copy.wait_send()

    @pl.when(has_above)
    def _():
        for copy in above_sent:
            copy.wait_send()

    for sems, send, recv in (
        (a_sem, send_a, recv_a),
        (b_sem, send_b, recv_b),
        (q_sem, send_q, recv_q),
        (o_sem, send_o, recv_o),
    ):
        for d in range(1, seqs):
            to = shard_at(d)
            remote(send.at[to], recv.at[me], sems, to, me, (to, col)).wait_send()


def fused_body(
    byte_input,
    b_proj,
    c_proj,
    step_decay,
    skip_gain,
    out_weight,
    boundaries,
    counts,
    norm_gain,
    qkv_weight,
):
    seqs, groups = lax.axis_size("seq"), lax.axis_size("head")
    heads = step_decay.shape[0]
    width = byte_input.shape[1]
    lanes = width // heads
    state = b_proj.shape[1]
    rows = ROWS_DEV
    piece = rows // groups
    enc = out_weight.shape[1]
    pieces = boundaries.shape[1] // piece
    vmem = pl.BlockSpec(memory_space=pltpu.VMEM)
    hbm = pl.BlockSpec(memory_space=pl.ANY)
    dma = pltpu.SemaphoreType.DMA
    operands = (
        step_decay,
        byte_input,
        b_proj,
        counts.reshape(1, 1),
        boundaries,
        c_proj,
        skip_gain.reshape(1, -1),
        out_weight,
        norm_gain.reshape(1, -1),
        qkv_weight,
    )
    result = pl.pallas_call(
        functools.partial(fused, seqs, groups),
        out_shape=jax.ShapeDtypeStruct((rows, width), OUT_WIRE),
        in_specs=[hbm] * len(operands),
        out_specs=vmem,
        scratch_shapes=[pltpu.VMEM(array.shape, array.dtype) for array in operands]
        + [
            pltpu.VMEM((seqs, lanes + EXTRA, state), STATE_WIRE),
            pltpu.VMEM((seqs, lanes + EXTRA, state), STATE_WIRE),
            pltpu.VMEM((seqs, lanes, state), STATE_WIRE),
            pltpu.VMEM((seqs, lanes, state), STATE_WIRE),
            pltpu.VMEM((pieces, piece, enc), PART_WIRE),
            pltpu.VMEM((2 * groups, piece, enc), PART_WIRE),
            pltpu.VMEM((groups, piece, enc), BF16),
            pltpu.VMEM((seqs, rows + rows // 2, 2 * lanes), BF16),
            pltpu.VMEM((seqs, rows + rows // 2, 2 * lanes), BF16),
            pltpu.VMEM((seqs, rows // 2, 2 * lanes), OUT_WIRE),
            pltpu.VMEM((seqs, rows // 2, 2 * lanes), OUT_WIRE),
            dma((len(operands),)),
            dma((2, seqs)),
            dma((2, seqs)),
            dma((2 * groups,)),
            dma((2 * groups,)),
            dma((2, groups)),
            dma((2, seqs)),
            dma((2, seqs)),
        ],
        compiler_params=pltpu.CompilerParams(collective_id=0, has_side_effects=True),
    )(*operands)
    return result.astype(F32)


def chosen(*args):
    byte_input, step_decay, slots = args[0], args[3], args[6].shape[1]
    heads = step_decay.shape[0]
    lanes = byte_input.shape[1] // heads
    seqs, groups = lax.axis_size("seq"), lax.axis_size("head")
    fits = seqs == heads and lanes == ATT_DIM and args[9].shape[2] == byte_input.shape[1]
    fits = fits and 2 * lanes == slots and args[1].shape[1] == slots and slots == 2 * ROWS_DEV
    fits = fits and seqs % 4 == 0 and groups % 2 == 0 and ROWS_DEV % (16 * groups) == 0
    fits = fits and byte_input.shape[0] % slots == 0
    return fused_body(*args) if fits else body(*args)


def solution(mesh):
    return jax.shard_map(
        chosen,
        mesh=mesh,
        in_specs=(
            P("seq", "head"),
            P("seq", None),
            P("seq", None),
            P("head", "seq"),
            P("head"),
            P("head", None),
            P("seq", None),
            P("seq"),
            P(),
            P(None, None, "head"),
        ),
        out_specs=P("seq", "head"),
        check_vma=False,
    )
```

```python
import functools

import jax
import jax.numpy as jnp
from jax import lax
from jax.experimental import pallas as pl
from jax.experimental.pallas import tpu as pltpu
from jax.sharding import PartitionSpec as P

ATT_DIM = 64
ROWS_DEV = 64


def prefix(shard, axis, combine, identity):
    length, here = (lax.axis_size(axis), lax.axis_index(axis))
    everything = jax.tree.map(lambda part: lax.all_gather(part, axis), shard)
    start = jax.tree.map(
        lambda part, zero: jnp.broadcast_to(jnp.asarray(zero, part.dtype), part.shape),
        shard,
        identity,
    )

    def lap(k, before):
        reached = k < here
        new = combine(before, jax.tree.map(lambda part: part[k], everything))
        return jax.tree.map(lambda a, b: jnp.where(reached, a, b), new, before)

    return lax.fori_loop(0, length, lap, start)


def extended(cells, sides, width):
    for axis, dim in sides:
        count = lax.axis_size(axis)
        ends = count - 1
        head = lax.slice_in_dim(cells, 0, width, axis=dim)
        tail = lax.slice_in_dim(cells, cells.shape[dim] - width, cells.shape[dim], axis=dim)
        cells = jnp.concatenate(
            [
                lax.ppermute(tail, axis, [(i, (i + 1) % count) for i in range(ends)]),
                cells,
                lax.ppermute(head, axis, [((i + 1) % count, i) for i in range(ends)]),
            ],
            axis=dim,
        )
    return cells


def state_space(inputs, b_rows, c_rows, decay):
    log_decay = jnp.cumsum(-decay, axis=1)
    affinity = jnp.dot(c_rows, b_rows.T, precision=lax.Precision.HIGHEST)
    length = inputs.shape[0]
    causal = lax.broadcasted_iota(jnp.int32, (length, length), 0) >= lax.broadcasted_iota(
        jnp.int32, (length, length), 1
    )

    def one_head(pair):
        values, logs = pair
        weights = (
            jnp.where(causal, jnp.exp(jnp.where(causal, logs[:, None] - logs[None, :], 0.0)), 0.0)
            * affinity
        )
        return jnp.dot(weights, values, precision=lax.Precision.HIGHEST)

    inside = lax.map(one_head, (inputs.transpose(1, 0, 2), log_decay))
    tail = jnp.exp(log_decay[:, -1:] - log_decay)
    own_state = jnp.einsum("ht,thp,tn->hpn", tail, inputs, b_rows, precision=lax.Precision.HIGHEST)
    return (log_decay, inside, own_state)


def link(earlier, later):
    return (earlier[0] * later[0], later[0][:, None, None] * earlier[1] + later[1])


def body(
    byte_input,
    b_proj,
    c_proj,
    step_decay,
    skip_gain,
    out_weight,
    boundaries,
    counts,
    norm_gain,
    qkv_weight,
):
    heads_here = step_decay.shape[0]
    length = byte_input.shape[0]
    inputs = byte_input.reshape(length, heads_here, -1)
    log_decay, inside, own_state = state_space(inputs, b_proj, c_proj, step_decay)
    span_decay = jnp.exp(log_decay[:, -1])
    arriving = prefix(
        (span_decay, own_state), "seq", link, (jnp.ones_like(span_decay), jnp.zeros_like(own_state))
    )
    carried = jnp.exp(log_decay)[:, :, None] * jnp.einsum(
        "tn,hpn->htp", c_proj, arriving[1], precision=lax.Precision.HIGHEST
    )
    mixed_heads = inside + carried + skip_gain[:, None, None] * inputs.transpose(1, 0, 2)
    slots = boundaries.shape[1]
    picked = jnp.take(mixed_heads, boundaries[0], axis=1)
    selected = picked.transpose(1, 0, 2).reshape(slots, -1).astype(jnp.bfloat16)
    all_counts = lax.all_gather(counts, "seq", axis=0, tiled=True)
    starts = jnp.cumsum(all_counts) - all_counts
    myself = lax.axis_index("seq")
    shards = lax.axis_size("seq")
    slot = jnp.arange(slots, dtype=jnp.int32)

    def slot_index(source):
        inside_axis = (source >= 0) & (source < shards)
        safe = jnp.clip(source, 0, shards - 1)
        begin = jnp.take(starts, safe)
        number = jnp.take(all_counts, safe)
        return jnp.where(inside_axis & (slot < number), begin + slot, -1)

    global_index = jnp.concatenate(
        [slot_index(myself - 1), slot_index(myself), slot_index(myself + 1)]
    )
    first_row = myself * ROWS_DEV
    target = first_row + jnp.arange(ROWS_DEV, dtype=jnp.int32)
    picker = global_index[None, :] == target[:, None]
    nearby = extended(selected, (("seq", 0),), slots)
    owned = jnp.dot(picker.astype(jnp.bfloat16), nearby, preferred_element_type=jnp.float32).astype(
        jnp.bfloat16
    )
    partial_value = jnp.dot(owned, out_weight, preferred_element_type=jnp.float32)
    packed = lax.psum(partial_value, "head")
    normed = (
        packed * lax.rsqrt(jnp.mean(packed * packed, axis=-1, keepdims=True) + 1e-05) * norm_gain
    ).astype(jnp.bfloat16)
    query = jnp.dot(normed, qkv_weight[0], preferred_element_type=jnp.float32).astype(jnp.bfloat16)
    keyed = jnp.dot(normed, qkv_weight[1], preferred_element_type=jnp.float32).astype(jnp.bfloat16)
    valued = jnp.dot(normed, qkv_weight[2], preferred_element_type=jnp.float32).astype(jnp.bfloat16)
    att_here = query.shape[1] // ATT_DIM
    queries = query.reshape(ROWS_DEV, att_here, ATT_DIM)
    row_place = first_row + jnp.arange(ROWS_DEV, dtype=jnp.int32)
    scale = ATT_DIM ** (-0.5)
    running = jnp.full((att_here, ROWS_DEV), -1e30, jnp.float32)
    key_piece = lax.all_gather(keyed, "seq", axis=0, tiled=True)
    value_piece = lax.all_gather(valued, "seq", axis=0, tiled=True)
    count = key_piece.shape[0]
    key_heads = key_piece.reshape(count, att_here, ATT_DIM)
    value_heads = value_piece.reshape(count, att_here, ATT_DIM)
    scores = (
        jnp.einsum("qhd,khd->hqk", queries, key_heads, preferred_element_type=jnp.float32) * scale
    )
    allowed = jnp.arange(count, dtype=jnp.int32)[None, :] <= row_place[:, None]
    scores = jnp.where(allowed[None], scores, -1e30)
    highest = jnp.maximum(running, jnp.max(scores, axis=-1))
    exps = jnp.where(allowed[None], jnp.exp(scores - highest[:, :, None]), 0.0)
    totals = jnp.sum(exps, axis=-1)
    weights = exps.astype(jnp.bfloat16)
    accum = jnp.einsum("hqk,khd->hqd", weights, value_heads, preferred_element_type=jnp.float32)
    running, totals, accum = (highest, totals, accum)
    result = accum / totals[:, :, None]
    return result.transpose(1, 0, 2).reshape(ROWS_DEV, att_here * ATT_DIM)


F32 = jnp.float32
BF16 = jnp.bfloat16
STATE_WIRE = jnp.bfloat16
PART_WIRE = jnp.bfloat16
OUT_WIRE = jnp.bfloat16
EXTRA = 16


def exact_dot(a, b, dims=((1,), (0,))):
    return lax.dot_general(
        a, b, (dims, ((), ())), precision=lax.Precision.HIGHEST, preferred_element_type=F32
    )


def fast_dot(a, b, dims=((1,), (0,))):
    return lax.dot_general(a, b, (dims, ((), ())), preferred_element_type=F32)


def halves(a):
    high = a.astype(BF16)
    return high, (a - high.astype(F32)).astype(BF16)


def iota(shape, dim):
    return lax.broadcasted_iota(jnp.int32, shape, dim)


def fused(
    seqs,
    groups,
    decay_hbm,
    x_hbm,
    b_hbm,
    counts_hbm,
    bound_hbm,
    c_hbm,
    skip_hbm,
    outw_hbm,
    gain_hbm,
    qkvw_hbm,
    out_ref,
    decay_ref,
    x_ref,
    b_ref,
    counts_ref,
    bound_ref,
    c_ref,
    skip_ref,
    outw,
    gain_ref,
    qkvw,
    send_a,
    recv_a,
    send_b,
    recv_b,
    send_p,
    recv_p,
    recv_n,
    send_q,
    recv_q,
    send_o,
    recv_o,
    weight_sem,
    a_sem,
    b_sem,
    p_send,
    p_recv,
    n_sem,
    q_sem,
    o_sem,
):
    me = lax.axis_index("seq")
    col = lax.axis_index("head")
    length, width = x_ref.shape
    heads = decay_ref.shape[0]
    lanes = width // heads
    state = b_ref.shape[1]
    slots = bound_ref.shape[1]
    rows = out_ref.shape[0]
    piece = rows // groups
    half = rows // 2

    def shard_at(d):
        return lax.rem(me + d + seqs, seqs)

    layers = seqs // 2
    mid = layers // 2
    layer, side = me // 2, lax.rem(me, 2)
    near_end = layer < mid
    far_layers = [jnp.where(near_end, layers - 1 - k, k) for k in range(layers - mid)]
    same = jnp.where(near_end, layer, layer - (layers - mid))
    for k in range(1, mid):
        turn = lax.rem(same + k, mid)
        far_layers.append(jnp.where(near_end, turn, turn + (layers - mid)))
    targets = []
    for there in far_layers + [layer]:
        targets.append(2 * there + 1 - side)
        if there is not layer:
            targets.append(2 * there + side)

    def head_at(d):
        return lax.rem(col + d, groups)

    barrier = pltpu.get_barrier_semaphore()
    peers = [(shard_at(d), col) for d in range(1, seqs)]
    peers += [(me, head_at(d)) for d in range(1, groups)]
    peers += [(shard_at(e), head_at(d)) for e in (-1, 1) for d in range(1, groups)]
    for peer in peers:
        pl.semaphore_signal(
            barrier, inc=1, device_id=peer, device_id_type=pl.DeviceIdType.MESH
        )

    def remote(src, dst, sems, k, source, peer):
        return pltpu.make_async_remote_copy(
            src_ref=src,
            dst_ref=dst,
            send_sem=sems.at[0, k],
            recv_sem=sems.at[1, source],
            device_id=peer,
            device_id_type=pl.DeviceIdType.MESH,
        )

    loads = [
        pltpu.make_async_copy(source, target, weight_sem.at[i])
        for i, (source, target) in enumerate(
            (
                (decay_hbm, decay_ref),
                (x_hbm, x_ref),
                (b_hbm, b_ref),
                (counts_hbm, counts_ref),
                (bound_hbm, bound_ref),
                (c_hbm, c_ref),
                (skip_hbm, skip_ref),
                (outw_hbm, outw),
                (gain_hbm, gain_ref),
                (qkvw_hbm, qkvw),
            )
        )
    ]
    for load in loads[:7]:
        load.start()

    loads[0].wait()
    decay = decay_ref[...]
    upper = (iota((length, length), 0) <= iota((length, length), 1)).astype(F32)
    lower = (iota((length, length), 0) >= iota((length, length), 1)).astype(F32)
    logs = -exact_dot(decay, upper)
    logs_t = -exact_dot(lower, decay, ((1,), (1,)))
    first = iota((heads, width), 0) * lanes
    channel = iota((heads, width), 1)
    spread = ((channel >= first) & (channel < first + lanes)).astype(F32)
    tail_t = jnp.exp(logs_t[length - 1 : length, :] - logs_t)
    loads[1].wait()
    loads[2].wait()
    loads[3].wait()
    for load in loads[7:]:
        load.start()
    scaled = x_ref[...] * exact_dot(tail_t, spread)
    own = exact_dot(scaled, b_ref[...], ((0,), (0,)))
    number = jnp.broadcast_to(counts_ref[...].astype(F32), (EXTRA, state))
    extra_row = iota((EXTRA, state), 0)
    for h in range(heads):
        send_a[h, :lanes, :] = own[h * lanes : (h + 1) * lanes, :].astype(send_a.dtype)
        last = jnp.broadcast_to(logs[h : h + 1, length - 1 : length], (EXTRA, state))
        last_high, rest = halves(last)
        rest = last - last_high.astype(F32)
        last_mid, last_low = halves(rest)
        extra = jnp.where(extra_row == 1, last_mid.astype(F32), last_high.astype(F32))
        extra = jnp.where(extra_row == 2, last_low.astype(F32), extra)
        extra = jnp.where(extra_row == 3, number, extra)
        send_a[h, lanes:, :] = extra.astype(send_a.dtype)
    pl.semaphore_wait(barrier, len(peers))
    for to in targets:
        remote(send_a.at[to], recv_a.at[me], a_sem, to, me, (to, col)).start()
    recv_a[me] = send_a[me]

    for load in loads[4:7]:
        load.wait()
    marks = jnp.broadcast_to(bound_ref[...].astype(F32), (slots, slots)).T
    marks = jnp.concatenate([marks] * (length // slots), axis=1)
    place = iota((slots, length), 1).astype(F32)
    hit = place == marks
    seen = place <= marks
    onehot = hit.astype(F32)
    c_rows = exact_dot(onehot, c_ref[...])
    logs_sel = exact_dot(onehot, logs_t)
    affinity = exact_dot(c_rows, b_ref[...], ((1,), (1,)))
    inside = []
    first_lane = iota((slots, 2 * lanes), 1) < lanes
    for pair in range(heads // 2):
        x_high, x_low = halves(x_ref[:, pair * 2 * lanes : (pair + 1) * 2 * lanes])
        x_both = jnp.concatenate([x_high, x_low], axis=1)
        parts = []
        for h in (2 * pair, 2 * pair + 1):
            gap = logs_sel[:, h : h + 1] - logs[h : h + 1, :]
            weights = jnp.where(seen, jnp.exp(jnp.where(seen, gap, 0.0)), 0.0) * affinity
            weights = weights + jnp.where(hit, skip_ref[:, h : h + 1], 0.0)
            w_high, w_low = halves(weights)
            wide = fast_dot(w_high, x_both)
            parts.append(
                wide[:, : 2 * lanes] + wide[:, 2 * lanes :] + fast_dot(w_low, x_high)
            )
        inside.append(jnp.where(first_lane, parts[0], parts[1]))
    inside = jnp.concatenate(inside, axis=1)
    enter_scale = exact_dot(jnp.exp(logs_sel), spread)

    for d in range(1, seqs):
        source = shard_at(-d)
        copy = remote(send_a.at[shard_at(d)], recv_a.at[source], a_sem, source, source, (source, col))
        copy.wait_recv()
    running = jnp.zeros((lanes, state), F32)
    for s in range(seqs):
        send_b[s] = running.astype(send_b.dtype)
        if s < seqs - 1:
            tags = recv_a[s, lanes:, :].astype(F32)
            kept = jnp.exp((tags[0:1] + tags[1:2]) + tags[2:3])
            running = kept * running + recv_a[s, :lanes, :].astype(F32)
    for to in targets:
        remote(send_b.at[to], recv_b.at[me], b_sem, to, me, (to, col)).start()
    recv_b[me] = send_b[me]

    start = jnp.zeros((1, state), F32)
    for s in range(seqs):
        start = start + jnp.where(s < me, recv_a[s, lanes:, :].astype(F32)[3:4], 0.0)
    offset = start - (me * rows - half).astype(F32)
    slot = iota((slots, slots), 1).astype(F32)
    mine = jnp.broadcast_to(counts_ref[...].astype(F32), (slots, slots))
    shift = (slot == iota((slots, slots), 0).astype(F32) - offset) & (slot < mine)
    shift = shift.astype(BF16)

    for d in range(1, seqs):
        source = shard_at(-d)
        remote(send_b.at[shard_at(d)], recv_b.at[source], b_sem, source, source, (source, col)).wait_recv()
    entering = recv_b[...].reshape(heads * lanes, state)
    c_high, c_low = halves(c_rows)
    last_dims = ((1,), (1,))
    carried = fast_dot(c_high, entering, last_dims) + fast_dot(c_low, entering, last_dims)
    y = (inside + enter_scale * carried).astype(BF16)
    window = fast_dot(shift, y).astype(BF16)
    loads[7].wait()
    partial = fast_dot(window, outw[...])
    pieces = slots // piece
    for i in range(pieces):
        send_p[i] = partial[i * piece : (i + 1) * piece, :].astype(send_p.dtype)
    outer = (pieces - groups) // 2

    def project(src, slot, k, peer):
        return pltpu.make_async_remote_copy(
            src_ref=send_p.at[src],
            dst_ref=recv_p.at[slot],
            send_sem=p_send.at[k],
            recv_sem=p_recv.at[slot],
            device_id=peer,
            device_id_type=pl.DeviceIdType.MESH,
        )

    below_sent = [project(i, groups + col, i, (shard_at(-1), groups - outer + i)) for i in range(outer)]
    above_sent = [
        project(outer + groups + i, groups + col, outer + i, (shard_at(1), i))
        for i in range(outer)
    ]
    sent = []
    for d in range(1, groups):
        to = head_at(d)
        sent.append(project(outer + to, col, 2 * outer + d - 1, (me, to)))
    has_below, has_above = me > 0, me < seqs - 1

    @pl.when(has_below)
    def _():
        for copy in below_sent:
            copy.start()

    @pl.when(has_above)
    def _():
        for copy in above_sent:
            copy.start()

    for copy in sent:
        copy.start()
    recv_p[col] = send_p[outer + col]
    expects = (has_below & (col < outer)) | (has_above & (col >= outer))

    @pl.when(expects)
    def _():
        for k in range(groups):
            project(0, groups + k, 0, (shard_at(1), k)).wait_recv()

    @pl.when(jnp.logical_not(expects))
    def _():
        recv_p[groups:] = jnp.zeros((groups, piece, recv_p.shape[2]), recv_p.dtype)

    for d in range(1, groups):
        source = head_at(groups - d)
        project(0, source, 0, (me, source)).wait_recv()
    loads[8].wait()
    mixed = recv_p[0].astype(F32)
    for k in range(1, 2 * groups):
        mixed = mixed + recv_p[k].astype(F32)
    square = jnp.mean(mixed * mixed, axis=-1, keepdims=True)
    normed = (mixed * lax.rsqrt(square + 1e-05) * gain_ref[...]).astype(BF16)
    recv_n[col] = normed
    sent_n = []
    for d in range(1, groups):
        to = head_at(d)
        sent_n.append(remote(recv_n.at[col], recv_n.at[col], n_sem, to, col, (me, to)))
        sent_n[-1].start()
    for d in range(1, groups):
        source = head_at(groups - d)
        remote(recv_n.at[col], recv_n.at[source], n_sem, source, source, (me, source)).wait_recv()
    normed = recv_n[...].reshape(rows, -1)
    loads[9].wait()
    query, key, value = [
        fast_dot(normed, qkvw[i]).astype(BF16).astype(F32) for i in range(3)
    ]
    pair_width = 2 * lanes
    left = iota((rows, pair_width), 1) < lanes
    left_half = left[:half]

    def turned(a):
        return pltpu.roll(a, lanes, 1)

    for pair in range(heads // 2):
        at = slice(pair * pair_width, (pair + 1) * pair_width)
        q, k, v = query[:, at], key[:, at], value[:, at]
        send_q[2 * pair, :rows, :] = jnp.where(left, q, turned(k)).astype(BF16)
        send_q[2 * pair + 1, :rows, :] = jnp.where(left, turned(q), k).astype(BF16)
        above, below = v[:half], v[half:]
        send_q[2 * pair, rows:, :] = jnp.where(left_half, above, turned(below)).astype(BF16)
        send_q[2 * pair + 1, rows:, :] = jnp.where(
            left_half, turned(above), below
        ).astype(BF16)
    for to in targets:
        remote(send_q.at[to], recv_q.at[me], q_sem, to, me, (to, col)).start()
    recv_q[me] = send_q[me]
    for d in range(1, seqs):
        source = shard_at(-d)
        remote(send_q.at[shard_at(d)], recv_q.at[source], q_sem, source, source, (source, col)).wait_recv()
    coarse = seqs * rows
    both = recv_q[:, :rows, :].reshape(coarse, pair_width)
    wide = both.astype(F32)
    left_all = iota((coarse, pair_width), 1) < lanes
    queries = jnp.where(left_all, wide, 0.0).astype(BF16)
    keys = turned(wide).astype(BF16)
    values = []
    for s in range(seqs):
        packed = recv_q[s, rows:, :].astype(F32)
        values += [packed, turned(packed)]
    values = jnp.concatenate(values, axis=0).astype(BF16)
    scores = fast_dot(queries, keys, ((1,), (1,))) * (lanes ** (-0.5))
    allowed = iota((coarse, coarse), 0) >= iota((coarse, coarse), 1)
    scores = jnp.where(allowed, scores, -1e30)
    highest = jnp.max(scores, axis=-1, keepdims=True)
    exps = jnp.where(allowed, jnp.exp(scores - highest), 0.0)
    total = jnp.sum(exps, axis=-1, keepdims=True)
    result = fast_dot(exps.astype(BF16), values) / total
    for s in range(seqs):
        above = result[s * rows : s * rows + half]
        below = result[s * rows + half : (s + 1) * rows]
        send_o[s] = jnp.where(left_half, above, turned(below)).astype(send_o.dtype)
    for to in targets:
        remote(send_o.at[to], recv_o.at[me], o_sem, to, me, (to, col)).start()
    recv_o[me] = send_o[me]
    for d in range(1, seqs):
        source = shard_at(-d)
        remote(send_o.at[shard_at(d)], recv_o.at[source], o_sem, source, source, (source, col)).wait_recv()
    for pair in range(heads // 2):
        at = slice(pair * pair_width, (pair + 1) * pair_width)
        even, odd = recv_o[2 * pair].astype(F32), recv_o[2 * pair + 1].astype(F32)
        out_ref[:half, at] = jnp.where(left_half, even, turned(odd)).astype(OUT_WIRE)
        out_ref[half:, at] = jnp.where(left_half, turned(even), odd).astype(OUT_WIRE)

    for copy in sent + sent_n:
        copy.wait_send()

    @pl.when(has_below)
    def _():
        for copy in below_sent:
            copy.wait_send()

    @pl.when(has_above)
    def _():
        for copy in above_sent:
            copy.wait_send()

    for sems, send, recv in (
        (a_sem, send_a, recv_a),
        (b_sem, send_b, recv_b),
        (q_sem, send_q, recv_q),
        (o_sem, send_o, recv_o),
    ):
        for d in range(1, seqs):
            to = shard_at(d)
            remote(send.at[to], recv.at[me], sems, to, me, (to, col)).wait_send()


def fused_body(
    byte_input,
    b_proj,
    c_proj,
    step_decay,
    skip_gain,
    out_weight,
    boundaries,
    counts,
    norm_gain,
    qkv_weight,
):
    seqs, groups = lax.axis_size("seq"), lax.axis_size("head")
    heads = step_decay.shape[0]
    width = byte_input.shape[1]
    lanes = width // heads
    state = b_proj.shape[1]
    rows = ROWS_DEV
    piece = rows // groups
    enc = out_weight.shape[1]
    pieces = boundaries.shape[1] // piece
    vmem = pl.BlockSpec(memory_space=pltpu.VMEM)
    hbm = pl.BlockSpec(memory_space=pl.ANY)
    dma = pltpu.SemaphoreType.DMA
    operands = (
        step_decay,
        byte_input,
        b_proj,
        counts.reshape(1, 1),
        boundaries,
        c_proj,
        skip_gain.reshape(1, -1),
        out_weight,
        norm_gain.reshape(1, -1),
        qkv_weight,
    )
    result = pl.pallas_call(
        functools.partial(fused, seqs, groups),
        out_shape=jax.ShapeDtypeStruct((rows, width), OUT_WIRE),
        in_specs=[hbm] * len(operands),
        out_specs=vmem,
        scratch_shapes=[pltpu.VMEM(array.shape, array.dtype) for array in operands]
        + [
            pltpu.VMEM((seqs, lanes + EXTRA, state), STATE_WIRE),
            pltpu.VMEM((seqs, lanes + EXTRA, state), STATE_WIRE),
            pltpu.VMEM((seqs, lanes, state), STATE_WIRE),
            pltpu.VMEM((seqs, lanes, state), STATE_WIRE),
            pltpu.VMEM((pieces, piece, enc), PART_WIRE),
            pltpu.VMEM((2 * groups, piece, enc), PART_WIRE),
            pltpu.VMEM((groups, piece, enc), BF16),
            pltpu.VMEM((seqs, rows + rows // 2, 2 * lanes), BF16),
            pltpu.VMEM((seqs, rows + rows // 2, 2 * lanes), BF16),
            pltpu.VMEM((seqs, rows // 2, 2 * lanes), OUT_WIRE),
            pltpu.VMEM((seqs, rows // 2, 2 * lanes), OUT_WIRE),
            dma((len(operands),)),
            dma((2, seqs)),
            dma((2, seqs)),
            dma((2 * groups,)),
            dma((2 * groups,)),
            dma((2, groups)),
            dma((2, seqs)),
            dma((2, seqs)),
        ],
        compiler_params=pltpu.CompilerParams(collective_id=0, has_side_effects=True),
    )(*operands)
    return result.astype(F32)


def chosen(*args):
    byte_input, step_decay, slots = args[0], args[3], args[6].shape[1]
    heads = step_decay.shape[0]
    lanes = byte_input.shape[1] // heads
    seqs, groups = lax.axis_size("seq"), lax.axis_size("head")
    fits = seqs == heads and lanes == ATT_DIM and args[9].shape[2] == byte_input.shape[1]
    fits = fits and 2 * lanes == slots and args[1].shape[1] == slots and slots == 2 * ROWS_DEV
    fits = fits and seqs % 4 == 0 and groups % 2 == 0 and ROWS_DEV % (16 * groups) == 0
    fits = fits and byte_input.shape[0] % slots == 0
    return fused_body(*args) if fits else body(*args)


def solution(mesh):
    return jax.shard_map(
        chosen,
        mesh=mesh,
        in_specs=(
            P("seq", "head"),
            P("seq", None),
            P("seq", None),
            P("head", "seq"),
            P("head"),
            P("head", None),
            P("seq", None),
            P("seq"),
            P(),
            P(None, None, "head"),
        ),
        out_specs=P("seq", "head"),
        check_vma=False,
    )
```
